32 devices in a mesh: seg: 8 (over z, core), head: 4 (over y, x).
Axes of the slice: x: 2, y: 2, z: 4, core: 2. Of those that a mesh axis runs over, the one named last changes fastest.
Arguments:
- inputs: bfloat16 [8, 256, 16384], P('seg', None, 'head'), may hold values from -6 to 6
- deltas: float32 [8, 256, 256], P('seg', 'head'), may hold values from 0.01 to 0.1
- rates: float32 [256], P('head'), may hold values from 0.001 to 2
- skips: float32 [256], P('head'), may hold values from 0.5 to 1.5
- writer: bfloat16 [8, 256, 1024], P('seg'), may hold values from -1.796875 to 1.796875
- reader: bfloat16 [8, 256, 1024], P('seg'), may hold values from -1.796875 to 1.796875
- grad_out: bfloat16 [8, 256, 16384], P('seg', None, 'head'), may hold values from -6 to 6
- parents: int32 [8], replicated, may hold values from -1 to 7, as said below
- levels: int32 [8], replicated, may hold values from 0 to 2, as said below
Outputs:
- outputs: bfloat16 [8, 256, 16384], P('seg', None, 'head')
- grad_inputs: bfloat16 [8, 256, 16384], P('seg', None, 'head')
- grad_deltas: float32 [8, 256, 256], P('seg', 'head')
- grad_writer: bfloat16 [8, 256, 1024], P('seg', 'head')
- grad_reader: bfloat16 [8, 256, 1024], P('seg', 'head')
The draws below stay inside these ranges and needn't reach their ends.
Inputs may be any that keep to these rules, and one draw needn't show every extreme that they name: `parents`: roots have parent -1 and level 0; every other segment's parent has a level one less than its own. A segment has at most four children, and some segment has level 2. levels[s] is the number of ancestors of segment s.
All inputs are finite; a program needn't handle non-finite values.
Results may differ from the reference program's by a relative error of at most 0.0046.
Values may be sent and summed in bfloat16 or wider, within the bound.
No kernel may reach another device: no remote copies, remote signals or barrier semaphores. Data moves between devices by JAX's collectives and lax.ppermute only.
A program may use at most 128 MiB of HBM per device.

```python
import math
import jax
import jax.numpy as jnp
from jax import lax

H = 256
P_SIZE = 64
N = 128
G = 8
SEG_LEN = 256
BLOCK = 256
DEPTH = 3
SEGS = 8


def tree_tables(key):
    counts = jax.random.randint(jax.random.fold_in(key, 11), (SEGS,), 2, 5).astype(jnp.int32)
    shuffled = jax.random.permutation(jax.random.fold_in(key, 12), SEGS).astype(jnp.int32)
    slots = jnp.arange(SEGS, dtype=jnp.int32)
    top_place = jnp.argmax((shuffled == SEGS - 1).astype(jnp.int32)).astype(jnp.int32)
    first_value = shuffled[0]
    order = shuffled.at[top_place].set(first_value).at[0].set(SEGS - 1)

    def place(number, carry):
        parent_bfs, level_bfs, current, remain = carry
        lowest = jnp.where(remain > 0, current, current + 1)
        usable = (slots >= lowest) & (slots < number) & (level_bfs < DEPTH - 1)
        picked = jnp.min(jnp.where(usable, slots, SEGS))
        found = picked < SEGS
        safe_pick = jnp.minimum(picked, SEGS - 1)
        same = picked == current
        new_remain = jnp.where(same, remain - 1, counts[safe_pick] - 1)
        new_current = jnp.where(same, current, safe_pick)
        parent_bfs = parent_bfs.at[number].set(jnp.where(found, safe_pick, -1))
        level_bfs = level_bfs.at[number].set(jnp.where(found, level_bfs[safe_pick] + 1, 0))
        current = jnp.where(found, new_current, current)
        remain = jnp.where(found, new_remain, remain)
        return (parent_bfs, level_bfs, current, remain)
    start_carry = (jnp.full((SEGS,), -1, jnp.int32), jnp.zeros((SEGS,), jnp.int32), jnp.int32(0), counts[0])
    parent_bfs, level_bfs, current, remain = lax.fori_loop(1, SEGS, place, start_carry)
    mapped = jnp.where(parent_bfs >= 0, order[jnp.maximum(parent_bfs, 0)], -1).astype(jnp.int32)
    parent_slot = jnp.zeros((SEGS,), jnp.int32).at[order].set(mapped)
    level_slot = jnp.zeros((SEGS,), jnp.int32).at[order].set(level_bfs)
    return (parent_slot, level_slot)


def draw_parents(key, part):
    return tree_tables(key)[0]


def draw_levels(key, part):
    return tree_tables(key)[1]


def shard_levels(own_key, shape, split, smallest, high):
    def one(axis_at, parts):
        draws = jax.random.uniform(jax.random.fold_in(jax.random.fold_in(own_key, 6), axis_at), (parts,), jnp.float32, smallest / len(split), high / len(split))
        return jnp.repeat(jnp.exp(draws), shape[axis_at] // parts).reshape((-1,) + (1,) * (len(shape) - axis_at - 1))

    loudness = one(*split[0])
    for cut in split[1:]:
        loudness = loudness * one(*cut)
    return loudness


def normal_values(stream_key, extent, deviation, limit, pieces=(), kind=jnp.bfloat16):
    factor_of = shard_levels(stream_key, extent, pieces, -0.22, 0.18) if pieces else 1.0
    drawn = jax.random.normal(stream_key, extent, jnp.float32) * deviation * factor_of
    return jnp.minimum(jnp.maximum(drawn, -limit), limit).astype(kind)


def setup_inputs(seed: int = 0) -> dict:
    splits = jax.random.split(jax.random.key(seed), 10)
    inputs = normal_values(splits[0], (SEGS, SEG_LEN, H * P_SIZE), 1.0, 6.0, ((0, 8), (2, 4)))
    deltas = jnp.clip(jnp.exp(math.log(0.1) - 2.3025851 * jax.random.uniform(splits[1], (SEGS, H, SEG_LEN), jnp.float32) ** shard_levels(splits[1], (SEGS, H, SEG_LEN), ((0, 8), (1, 4)), -0.2, 0.2)), 0.01, 0.1)
    rates = jnp.clip(jnp.exp(math.log(2.0) - 7.6009024 * jax.random.uniform(splits[2], (H,), jnp.float32) ** shard_levels(splits[2], (H,), ((0, 4),), -0.2, 0.2)), 0.001, 2.0)
    skips = jnp.clip(0.5 + 1.0 * jax.random.uniform(splits[3], (H,), jnp.float32) ** shard_levels(splits[3], (H,), ((0, 4),), -0.2, 0.2), 0.5, 1.5)
    writer = normal_values(splits[4], (SEGS, SEG_LEN, G * N), 0.3, 1.796875, ((0, 8),))
    reader = normal_values(splits[5], (SEGS, SEG_LEN, G * N), 0.3, 1.796875, ((0, 8),))
    grad_out = normal_values(splits[6], (SEGS, SEG_LEN, H * P_SIZE), 1.0, 6.0, ((0, 8), (2, 4)))
    parents = draw_parents(jax.random.fold_in(splits[9], 71), 0)
    levels = draw_levels(jax.random.fold_in(splits[9], 71), 0)
    return {"inputs": inputs, "deltas": deltas, "rates": rates, "skips": skips, "writer": writer, "reader": reader, "grad_out": grad_out, "parents": parents, "levels": levels}


exact_mode = lax.Precision.HIGHEST

def round_half(values):
    return lax.optimization_barrier(values.astype(jnp.bfloat16)).astype(jnp.float32)

def ssd_forward(values, deltas, rates, writer, reader, start, block):
    length, groups, per_group, width = values.shape
    state_size = writer.shape[-1]
    blocks = length // block
    log_decay = (-rates[:, :, None] * deltas).reshape(groups, per_group, blocks, block)
    within = jnp.cumsum(log_decay, axis=-1)
    value_blk = values.reshape(blocks, block, groups, per_group, width)
    write_blk = writer.reshape(blocks, block, groups, state_size)
    read_blk = reader.reshape(blocks, block, groups, state_size)
    delta_blk = deltas.reshape(groups, per_group, blocks, block)
    scores = jnp.einsum('cign,cjgn->gcij', read_blk, write_blk, precision=exact_mode)
    positions = jnp.arange(block)
    causal = positions[:, None] >= positions[None, :]
    log_gap = within[..., :, None] - within[..., None, :]
    decays = jnp.exp(jnp.where(causal, log_gap, -jnp.inf))
    weights = scores[:, None] * decays * delta_blk[..., None, :]
    within_out = jnp.einsum('ghcij,cjghp->cighp', weights, value_blk, precision=exact_mode)
    tail_decay = jnp.exp(within[..., -1:] - within) * delta_blk
    local_state = jnp.einsum('ghcj,cjghp,cjgn->cghpn', tail_decay, value_blk, write_blk, precision=exact_mode)
    totals = jnp.exp(within[..., -1])
    current = start
    outer_terms = []
    for number in range(blocks):
        read_out = jnp.einsum('ign,ghpn->ighp', read_blk[number], current, precision=exact_mode)
        scale_in = jnp.transpose(jnp.exp(within[:, :, number, :]), (2, 0, 1))
        outer_terms.append(read_out * scale_in[..., None])
        current = totals[:, :, number, None, None] * current + local_state[number]
    output = within_out + jnp.stack(outer_terms)
    return (output.reshape(length, groups, per_group, width), current)

def segment_end(values, deltas, rates, writer):
    running = jnp.cumsum(-rates[:, :, None] * deltas, axis=-1)
    total = running[..., -1]
    tail_decay = jnp.exp(total[..., None] - running) * deltas
    local_state = jnp.einsum('ghj,jghp,jgn->ghpn', tail_decay, values, writer, precision=exact_mode)
    return (local_state, jnp.exp(total))

def start_grad(grads, deltas, rates, reader):
    running = jnp.cumsum(-rates[:, :, None] * deltas, axis=-1)
    return jnp.einsum('ghi,ighp,ign->ghpn', jnp.exp(running), grads, reader, precision=exact_mode)

def reference(inputs, deltas, rates, skips, writer, reader, grad_out, parents, levels):
    per_group = H // G
    segments = inputs.shape[0]
    length = inputs.shape[1]
    rate_grid = rates.reshape(G, per_group)
    skip_grid = skips.reshape(G, per_group)

    def unpack(number):
        values = inputs[number].astype(jnp.float32).reshape(length, G, per_group, P_SIZE)
        delta_one = deltas[number].reshape(G, per_group, length)
        write_one = writer[number].astype(jnp.float32).reshape(length, G, N)
        read_one = reader[number].astype(jnp.float32).reshape(length, G, N)
        grads = grad_out[number].astype(jnp.float32).reshape(length, G, per_group, P_SIZE)
        return (values, delta_one, write_one, read_one, grads)

    def ends_of(number):
        values, delta_one, write_one, read_one, grads = unpack(number)
        local_state, decay_all = segment_end(values, delta_one, rate_grid, write_one)
        return (local_state, decay_all, start_grad(grads, delta_one, rate_grid, read_one))
    slots = jnp.arange(segments, dtype=jnp.int32)
    local_states, decay_all, start_parts = lax.map(ends_of, slots)
    is_root = (parents < 0)[:, None, None, None, None]
    safe_parent = jnp.maximum(parents, 0)
    starts = jnp.zeros_like(local_states)
    for repeat in range(DEPTH - 1):
        end_states = round_half(decay_all[..., None, None] * starts + local_states)
        at_level = (levels == repeat + 1)[:, None, None, None, None]
        starts = jnp.where(at_level, end_states[safe_parent], starts)
    grad_ends = jnp.zeros_like(local_states)
    for repeat in range(DEPTH - 1):
        grad_starts = decay_all[..., None, None] * grad_ends + start_parts
        grad_starts = jnp.where(is_root, 0.0, grad_starts)
        grad_ends = jax.ops.segment_sum(grad_starts, safe_parent, num_segments=segments)

    def backward(number):
        values, delta_one, write_one, read_one, grads = unpack(number)

        def core_map(values, delta_one, write_one, read_one):
            return ssd_forward(values, delta_one, rate_grid, write_one, read_one, starts[number], BLOCK)
        (core_out, end_state), pullback = jax.vjp(core_map, values, delta_one, write_one, read_one)
        grad_values, grad_delta, grad_write, grad_read = pullback((grads, grad_ends[number]))
        result = core_out + skip_grid[None, :, :, None] * values
        grad_values = grad_values + skip_grid[None, :, :, None] * grads
        return (result.reshape(length, H * P_SIZE).astype(jnp.bfloat16), grad_values.reshape(length, H * P_SIZE).astype(jnp.bfloat16), grad_delta.reshape(H, length), grad_write.reshape(length, G * N).astype(jnp.bfloat16), grad_read.reshape(length, G * N).astype(jnp.bfloat16))
    outputs, grad_inputs, grad_deltas, grad_writer, grad_reader = lax.map(backward, slots)
    return (outputs, grad_inputs, grad_deltas, grad_writer, grad_reader)
```

```python
import functools

import jax
import jax.numpy as jnp
from jax import lax
from jax.experimental import pallas as pl
from jax.experimental.pallas import tpu as pltpu
from jax.sharding import PartitionSpec as P

H = 256
P_SIZE = 64
N = 128
G = 8
DEPTH = 3
TILE = 256
SLOTS = 64

F32 = jnp.float32
BF16 = jnp.bfloat16


def dot(a, b, dims=((1,), (0,))):
    return lax.dot_general(a, b, (dims, ((), ())), preferred_element_type=F32)


NT = ((1,), (1,))


def split(value, parts):
    pieces = []
    for _ in range(parts):
        piece = value.astype(BF16)
        pieces.append(piece)
        value = value - piece.astype(F32)
    return pieces


def iota(shape, axis):
    return lax.broadcasted_iota(jnp.int32, shape, axis)


def onehot(cond):
    return jnp.where(cond, 1.0, 0.0).astype(BF16)


def spread(step):
    shape = (2 * SLOTS, TILE)
    head = step * (TILE // P_SIZE) + iota(shape, 1) // P_SIZE
    return onehot((iota(shape, 0) % SLOTS) == head)


def local_kernel(
    per_group,
    _,
    x_ref,
    dy_ref,
    delta_ref,
    rate_ref,
    b_ref,
    c_ref,
    u_ref,
    v_ref,
    xs_ref,
    ys_ref,
    table_ref,
    low_ref,
    up_ref,
    gb_ref,
    gc_ref,
    acc_ref,
):
    step = pl.program_id(0)
    length = x_ref.shape[0]
    square = (length, length)

    @pl.when(step == 0)
    def _():
        tri = onehot(iota(square, 0) >= iota(square, 1))
        eye = onehot(iota(square, 0) == iota(square, 1))
        pieces = split(delta_ref[...], 3)
        sums = sum(dot(tri, piece, NT) for piece in pieces)
        delta = sum(dot(eye, piece, NT) for piece in pieces)
        log = rate_ref[...] * sums
        grow = split(jnp.exp(log) * delta, 2)
        fall = split(jnp.exp(-log), 2)
        table_ref[0] = jnp.concatenate(fall, axis=1)
        table_ref[1] = jnp.concatenate(grow, axis=1)

    lanes = spread(step)
    fall = dot(table_ref[0], lanes)
    grow = dot(table_ref[1], lanes)
    xs, xs_low = split(x_ref[...].astype(F32) * grow, 2)
    ys, ys_low = split(dy_ref[...].astype(F32) * fall, 2)
    xs_ref[...] = xs
    ys_ref[...] = ys
    b, c = b_ref[...], c_ref[...]
    u = dot(b, xs, ((0,), (0,))) + dot(b, xs_low, ((0,), (0,)))
    v = dot(c, ys, ((0,), (0,))) + dot(c, ys_low, ((0,), (0,)))
    u_ref[...] = (u * fall[length - 1 :]).astype(BF16)
    v_ref[...] = v.astype(BF16)
    part = dot(ys, xs, NT)
    inner = step % per_group

    @pl.when(inner == 0)
    def _():
        acc_ref[...] = part

    @pl.when(inner > 0)
    def _():
        acc_ref[...] += part

    @pl.when(inner == per_group - 1)
    def _():
        lower = iota(square, 0) >= iota(square, 1)
        upper = iota(square, 0) <= iota(square, 1)
        low_ref[...] = jnp.where(lower, dot(c, b, NT), 0.0).astype(BF16)
        up_ref[...] = jnp.where(upper, dot(b, c, NT), 0.0).astype(BF16)
        high, low = split(jnp.where(lower, acc_ref[...], 0.0), 2)
        gc_ref[...] = dot(high, b) + dot(low, b)
        gb_ref[...] = dot(high, c, ((0,), (0,))) + dot(low, c, ((0,), (0,)))


def local_part(x, dy, delta, rate, writer, reader, first_group, local_groups):
    length, lanes = x.shape
    steps = lanes // TILE
    per_group = steps // local_groups
    tile = lambda rows: pl.BlockSpec((rows, TILE), lambda i, f: (0, i))
    whole = lambda *shape: pl.BlockSpec(shape, lambda i, f: (0,) * len(shape))
    group = lambda rows, cols: pl.BlockSpec((None, rows, cols), lambda i, f: (i // per_group, 0, 0))
    proj = pl.BlockSpec((length, N), lambda i, f: (0, f[0] + i // per_group))
    shape = jax.ShapeDtypeStruct
    return pl.pallas_call(
        functools.partial(local_kernel, per_group),
        grid_spec=pltpu.PrefetchScalarGridSpec(
            num_scalar_prefetch=1,
            grid=(steps,),
            in_specs=[
                tile(length),
                tile(length),
                whole(SLOTS, length),
                whole(1, SLOTS),
                proj,
                proj,
            ],
            out_specs=[
                tile(N),
                tile(N),
                tile(length),
                tile(length),
                whole(2, length, 2 * SLOTS),
                group(length, length),
                group(length, length),
                group(length, N),
                group(length, N),
            ],
            scratch_shapes=[pltpu.VMEM((length, length), F32)],
        ),
        out_shape=[
            shape((N, lanes), BF16),
            shape((N, lanes), BF16),
            shape((length, lanes), BF16),
            shape((length, lanes), BF16),
            shape((2, length, 2 * SLOTS), BF16),
            shape((local_groups, length, length), BF16),
            shape((local_groups, length, length), BF16),
            shape((local_groups, length, N), F32),
            shape((local_groups, length, N), F32),
        ],
        cost_estimate=pl.CostEstimate(
            flops=8 * length * lanes * length, transcendentals=0, bytes_accessed=12 * length * lanes
        ),
        name="local_part",
    )(first_group, x, dy, delta, rate, writer, reader)


def final_kernel(
    per_group,
    steps,
    _,
    x_ref,
    dy_ref,
    xs_ref,
    ys_ref,
    start_ref,
    end_ref,
    u_ref,
    table_ref,
    low_ref,
    up_ref,
    b_ref,
    c_ref,
    gb_in,
    gc_in,
    skip_ref,
    delta_ref,
    rate_ref,
    out_ref,
    dx_ref,
    gb_ref,
    gc_ref,
    dd_ref,
    sums_ref,
    accb_ref,
    accc_ref,
):
    step = pl.program_id(0)
    length = x_ref.shape[0]
    lanes = spread(step)
    fall = dot(table_ref[0], lanes)
    grow = dot(table_ref[1], lanes)
    xs, ys, start = xs_ref[...], ys_ref[...], start_ref[...]
    total = fall[length - 1 :]
    end = end_ref[...].astype(F32) * total
    end_high, end_low = split(end, 2)
    core = dot(low_ref[...], xs) + dot(c_ref[...], start)
    grad = dot(up_ref[...], ys) + dot(b_ref[...], end_high) + dot(b_ref[...], end_low)
    skip = skip_ref[...]
    out_ref[...] = (fall * core + skip * x_ref[...].astype(F32)).astype(out_ref.dtype)
    dx_ref[...] = (grow * grad + skip * dy_ref[...].astype(F32)).astype(dx_ref.dtype)

    inner = step % per_group

    @pl.when(inner == 0)
    def _():
        accb_ref[...] = gb_in[...]
        accc_ref[...] = gc_in[...]

    accc_ref[...] += dot(ys, start, NT)
    accb_ref[...] += dot(xs, end_high, NT) + dot(xs, end_low, NT)

    @pl.when(inner == per_group - 1)
    def _():
        gb_ref[...] = accb_ref[...].astype(gb_ref.dtype)
        gc_ref[...] = accc_ref[...].astype(gc_ref.dtype)

    direct = xs.astype(F32) * grad
    through = ys.astype(F32) * core - direct
    shape = (TILE, 2 * SLOTS)
    column = iota(shape, 1)
    head = step * (TILE // P_SIZE) + iota(shape, 0) // P_SIZE
    pick_through = onehot(column == head)
    pick_direct = onehot(column == head + SLOTS)
    high, low = split(through, 2)
    dhigh, dlow = split(direct, 2)
    rows = dot(high, pick_through) + dot(low, pick_through)
    rows = rows + dot(dhigh, pick_direct) + dot(dlow, pick_direct)

    @pl.when(step == 0)
    def _():
        sums_ref[...] = rows

    @pl.when(step > 0)
    def _():
        sums_ref[...] += rows

    held = u_ref[...].astype(F32) / total + start.astype(F32)
    last = jnp.sum(end * held, axis=0, keepdims=True)
    at_last = jnp.where(iota((8, TILE), 0) == 7, last, 0.0)
    high, low = split(at_last, 2)
    sums_ref[length - 8 :, :] += dot(high, pick_through) + dot(low, pick_through)

    @pl.when(step == steps - 1)
    def _():
        both = sums_ref[...].T
        square = (length, length)
        later = onehot(iota(square, 0) >= iota(square, 1))
        back = sum(dot(piece, later) for piece in split(both[:SLOTS], 3))
        dd_ref[...] = both[SLOTS:] / delta_ref[...] - rate_ref[...] * back


def final_part(
    x, dy, xs, ys, start, end, u, table, low, up, gb, gc, skip, delta, rate, writer, reader, first_group, grad_dtype
):
    length, lanes = x.shape
    steps = lanes // TILE
    local_groups = low.shape[0]
    per_group = steps // local_groups
    tile = lambda rows: pl.BlockSpec((rows, TILE), lambda i, f: (0, i))
    whole = lambda *shape: pl.BlockSpec(shape, lambda i, f: (0,) * len(shape))
    group = lambda rows, cols: pl.BlockSpec((None, rows, cols), lambda i, f: (i // per_group, 0, 0))
    proj = pl.BlockSpec((length, N), lambda i, f: (0, f[0] + i // per_group))
    shape = jax.ShapeDtypeStruct
    return pl.pallas_call(
        functools.partial(final_kernel, per_group, steps),
        grid_spec=pltpu.PrefetchScalarGridSpec(
            num_scalar_prefetch=1,
            grid=(steps,),
            in_specs=[
                tile(length),
                tile(length),
                tile(length),
                tile(length),
                tile(N),
                tile(N),
                tile(N),
                whole(2, length, 2 * SLOTS),
                group(length, length),
                group(length, length),
                proj,
                proj,
                group(length, N),
                group(length, N),
                tile(1),
                whole(SLOTS, length),
                whole(SLOTS, 1),
            ],
            out_specs=[
                tile(length),
                tile(length),
                pl.BlockSpec((length, N), lambda i, f: (0, i // per_group)),
                pl.BlockSpec((length, N), lambda i, f: (0, i // per_group)),
                whole(SLOTS, length),
            ],
            scratch_shapes=[
                pltpu.VMEM((length, 2 * SLOTS), F32),
                pltpu.VMEM((length, N), F32),
                pltpu.VMEM((length, N), F32),
            ],
        ),
        out_shape=[
            shape((length, lanes), BF16),
            shape((length, lanes), BF16),
            shape((length, local_groups * N), grad_dtype),
            shape((length, local_groups * N), grad_dtype),
            shape((SLOTS, length), F32),
        ],
        cost_estimate=pl.CostEstimate(
            flops=12 * length * lanes * length, transcendentals=0, bytes_accessed=16 * length * lanes
        ),
        name="final_part",
    )(
        first_group, x, dy, xs, ys, start, end, u, table, low, up, writer, reader, gb, gc, skip, delta, rate
    )


def tree_states(u, v, decay, parents, levels):
    segs = lax.axis_size("seg")
    lanes = u.shape[1]
    chunk = lanes // segs

    def spread_heads(state):
        parts = jnp.swapaxes(state.reshape(N, segs, chunk), 0, 1)
        return lax.all_to_all(parts, "seg", 0, 0)

    decay_all = lax.all_to_all(decay.reshape(segs, chunk), "seg", 0, 0)[:, None, :]
    u_all = spread_heads(u)
    v_all = spread_heads(v).astype(F32)
    safe = jnp.maximum(parents, 0)
    starts = jnp.zeros_like(u_all)
    for repeat in range(DEPTH - 1):
        ends = (decay_all * starts.astype(F32) + u_all.astype(F32)).astype(BF16)
        starts = jnp.where((levels == repeat + 1)[:, None, None], ends[safe], starts)
    link = (parents[None, :] == jnp.arange(segs)[:, None]).astype(F32)
    grad_end = jnp.zeros_like(v_all)
    for repeat in range(DEPTH - 1):
        lifted = decay_all * grad_end + v_all
        grad_end = sum(link[:, c, None, None] * lifted[c][None] for c in range(segs))

    def gather_heads(state):
        parts = lax.all_to_all(state, "seg", 0, 0)
        return jnp.swapaxes(parts, 0, 1).reshape(N, lanes)

    return gather_heads(starts), gather_heads(grad_end.astype(BF16))


def group_grads(gb, gc, members):
    shards_ = lax.axis_size("head")
    both = jnp.stack([gb, gc])
    length, width = gb.shape
    parts = both.reshape(2, shards_, length // shards_, width)
    parts = lax.all_to_all(parts, "head", 1, 1)
    if members > 1:
        parts = parts.reshape(2, shards_ // members, members, length // shards_, width).sum(2)
    parts = jnp.swapaxes(parts, 1, 2).reshape(2, length // shards_, -1)
    return parts.astype(BF16)


def shards(inputs, deltas, rates, skips, writer, reader, grad_out, parents, levels):
    heads = deltas.shape[1]
    per_group_all = H // G
    local_groups = max(1, heads // per_group_all)
    members = max(1, per_group_all // heads)
    first_group = (lax.axis_index("head") * heads // per_group_all).astype(jnp.int32)[None]
    x, dy = inputs[0], grad_out[0]
    pad = SLOTS - heads
    delta = jnp.pad(deltas[0], ((0, pad), (0, 0)))
    rate = jnp.pad(rates, (0, pad))
    u, v, xs, ys, table, low, up, gb, gc = local_part(
        x, dy, delta, rate[None, :], writer[0], reader[0], first_group, local_groups
    )
    decay = jnp.repeat(jnp.exp(-rates * jnp.sum(deltas[0], axis=1)), P_SIZE)
    start, end = tree_states(u, v, decay, parents, levels)
    out, dx, gb, gc, dd = final_part(
        x,
        dy,
        xs,
        ys,
        start,
        end,
        u,
        table,
        low,
        up,
        gb,
        gc,
        jnp.repeat(skips, P_SIZE)[None, :],
        delta,
        rate[:, None],
        writer[0],
        reader[0],
        first_group,
        BF16 if members == 1 else F32,
    )
    grads = group_grads(gb, gc, members)
    return (out[None], dx[None], dd[None, :heads], grads[0][None], grads[1][None])


def solution(mesh):
    placed = (
        P("seg", None, "head"),
        P("seg", "head", None),
        P("head"),
        P("head"),
        P("seg", None, None),
        P("seg", None, None),
        P("seg", None, "head"),
        P(),
        P(),
    )
    return jax.shard_map(
        shards,
        mesh=mesh,
        in_specs=placed,
        out_specs=(
            P("seg", None, "head"),
            P("seg", None, "head"),
            P("seg", "head", None),
            P("seg", "head", None),
            P("seg", "head", None),
        ),
        check_vma=False,
    )
```

```python
import functools

import jax
import jax.numpy as jnp
from jax import lax
from jax.experimental import pallas as pl
from jax.experimental.pallas import tpu as pltpu
from jax.sharding import PartitionSpec as P

H = 256
P_SIZE = 64
N = 128
G = 8
DEPTH = 3
TILE = 256
SLOTS = 64
EXTRA = 16

F32 = jnp.float32
BF16 = jnp.bfloat16


def dot(a, b, dims=((1,), (0,))):
    return lax.dot_general(a, b, (dims, ((), ())), preferred_element_type=F32)


NT = ((1,), (1,))


def split(value, parts):
    pieces = []
    for _ in range(parts):
        piece = value.astype(BF16)
        pieces.append(piece)
        value = value - piece.astype(F32)
    return pieces


def iota(shape, axis):
    return lax.broadcasted_iota(jnp.int32, shape, axis)


def onehot(cond):
    return jnp.where(cond, 1.0, 0.0).astype(BF16)


def spread(step):
    shape = (2 * SLOTS, TILE)
    head = step * (TILE // P_SIZE) + iota(shape, 1) // P_SIZE
    return onehot((iota(shape, 0) % SLOTS) == head)


def local_kernel(
    per_group,
    _,
    x_ref,
    dy_ref,
    delta_ref,
    rate_ref,
    b_ref,
    c_ref,
    u_ref,
    v_ref,
    xs_ref,
    ys_ref,
    table_ref,
    low_ref,
    up_ref,
    gb_ref,
    gc_ref,
    acc_ref,
):
    step = pl.program_id(0)
    length = x_ref.shape[0]
    square = (length, length)

    @pl.when(step == 0)
    def _():
        tri = onehot(iota(square, 0) >= iota(square, 1))
        eye = onehot(iota(square, 0) == iota(square, 1))
        pieces = split(delta_ref[...], 3)
        sums = sum(dot(tri, piece, NT) for piece in pieces)
        delta = sum(dot(eye, piece, NT) for piece in pieces)
        log = rate_ref[...] * sums
        grow = split(jnp.exp(log) * delta, 2)
        fall = split(jnp.exp(-log), 2)
        table_ref[0] = jnp.concatenate(fall, axis=1)
        table_ref[1] = jnp.concatenate(grow, axis=1)

    lanes = spread(step)
    fall = dot(table_ref[0], lanes)
    grow = dot(table_ref[1], lanes)
    xs, xs_low = split(x_ref[...].astype(F32) * grow, 2)
    ys, ys_low = split(dy_ref[...].astype(F32) * fall, 2)
    xs_ref[...] = xs
    ys_ref[...] = ys
    b, c = b_ref[...], c_ref[...]
    u = dot(b, xs, ((0,), (0,))) + dot(b, xs_low, ((0,), (0,)))
    v = dot(c, ys, ((0,), (0,))) + dot(c, ys_low, ((0,), (0,)))
    u_ref[...] = (u * fall[length - 1 :]).astype(BF16)
    v_ref[...] = v.astype(BF16)
    part = dot(ys, xs, NT)
    inner = step % per_group

    @pl.when(inner == 0)
    def _():
        acc_ref[...] = part

    @pl.when(inner > 0)
    def _():
        acc_ref[...] += part

    @pl.when(inner == per_group - 1)
    def _():
        lower = iota(square, 0) >= iota(square, 1)
        upper = iota(square, 0) <= iota(square, 1)
        low_ref[...] = jnp.where(lower, dot(c, b, NT), 0.0).astype(BF16)
        up_ref[...] = jnp.where(upper, dot(b, c, NT), 0.0).astype(BF16)
        high, low = split(jnp.where(lower, acc_ref[...], 0.0), 2)
        gc_ref[...] = dot(high, b) + dot(low, b)
        gb_ref[...] = dot(high, c, ((0,), (0,))) + dot(low, c, ((0,), (0,)))


def local_part(x, dy, delta, rate, writer, reader, first_group, local_groups):
    length, lanes = x.shape
    steps = lanes // TILE
    per_group = steps // local_groups
    tile = lambda rows: pl.BlockSpec((rows, TILE), lambda i, f: (0, i))
    whole = lambda *shape: pl.BlockSpec(shape, lambda i, f: (0,) * len(shape))
    group = lambda rows, cols: pl.BlockSpec((None, rows, cols), lambda i, f: (i // per_group, 0, 0))
    proj = pl.BlockSpec((length, N), lambda i, f: (0, f[0] + i // per_group))
    shape = jax.ShapeDtypeStruct
    return pl.pallas_call(
        functools.partial(local_kernel, per_group),
        grid_spec=pltpu.PrefetchScalarGridSpec(
            num_scalar_prefetch=1,
            grid=(steps,),
            in_specs=[
                tile(length),
                tile(length),
                whole(SLOTS, length),
                whole(1, SLOTS),
                proj,
                proj,
            ],
            out_specs=[
                tile(N),
                tile(N),
                tile(length),
                tile(length),
                whole(2, length, 2 * SLOTS),
                group(length, length),
                group(length, length),
                group(length, N),
                group(length, N),
            ],
            scratch_shapes=[pltpu.VMEM((length, length), F32)],
        ),
        out_shape=[
            shape((N, lanes), BF16),
            shape((N, lanes), BF16),
            shape((length, lanes), BF16),
            shape((length, lanes), BF16),
            shape((2, length, 2 * SLOTS), BF16),
            shape((local_groups, length, length), BF16),
            shape((local_groups, length, length), BF16),
            shape((local_groups, length, N), F32),
            shape((local_groups, length, N), F32),
        ],
        cost_estimate=pl.CostEstimate(
            flops=8 * length * lanes * length, transcendentals=0, bytes_accessed=12 * length * lanes
        ),
        name="local_part",
    )(first_group, x, dy, delta, rate, writer, reader)


def final_kernel(
    per_group,
    steps,
    _,
    x_ref,
    dy_ref,
    xs_ref,
    ys_ref,
    start_ref,
    end_ref,
    u_ref,
    table_ref,
    low_ref,
    up_ref,
    b_ref,
    c_ref,
    gb_in,
    gc_in,
    skip_ref,
    delta_ref,
    rate_ref,
    out_ref,
    dx_ref,
    gb_ref,
    gc_ref,
    dd_ref,
    sums_ref,
    accb_ref,
    accc_ref,
):
    step = pl.program_id(0)
    length = x_ref.shape[0]
    lanes = spread(step)
    fall = dot(table_ref[0], lanes)
    grow = dot(table_ref[1], lanes)
    xs, ys, start = xs_ref[...], ys_ref[...], start_ref[...]
    total = fall[length - 1 :]
    end = end_ref[...].astype(F32) * total
    end_high, end_low = split(end, 2)
    core = dot(low_ref[...], xs) + dot(c_ref[...], start)
    grad = dot(up_ref[...], ys) + dot(b_ref[...], end_high) + dot(b_ref[...], end_low)
    skip = skip_ref[...]
    out_ref[...] = (fall * core + skip * x_ref[...].astype(F32)).astype(out_ref.dtype)
    dx_ref[...] = (grow * grad + skip * dy_ref[...].astype(F32)).astype(dx_ref.dtype)

    inner = step % per_group

    @pl.when(inner == 0)
    def _():
        accb_ref[...] = gb_in[...]
        accc_ref[...] = gc_in[...]

    accc_ref[...] += dot(ys, start, NT)
    accb_ref[...] += dot(xs, end_high, NT) + dot(xs, end_low, NT)

    @pl.when(inner == per_group - 1)
    def _():
        gb_ref[...] = accb_ref[...].astype(gb_ref.dtype)
        gc_ref[...] = accc_ref[...].astype(gc_ref.dtype)

    direct = xs.astype(F32) * grad
    through = ys.astype(F32) * core - direct
    shape = (TILE, 2 * SLOTS)
    column = iota(shape, 1)
    head = step * (TILE // P_SIZE) + iota(shape, 0) // P_SIZE
    pick_through = onehot(column == head)
    pick_direct = onehot(column == head + SLOTS)
    high, low = split(through, 2)
    dhigh, dlow = split(direct, 2)
    rows = dot(high, pick_through) + dot(low, pick_through)
    rows = rows + dot(dhigh, pick_direct) + dot(dlow, pick_direct)

    @pl.when(step == 0)
    def _():
        sums_ref[...] = rows

    @pl.when(step > 0)
    def _():
        sums_ref[...] += rows

    held = u_ref[...].astype(F32) / total + start.astype(F32)
    last = jnp.sum(end * held, axis=0, keepdims=True)
    at_last = jnp.where(iota((8, TILE), 0) == 7, last, 0.0)
    high, low = split(at_last, 2)
    sums_ref[length - 8 :, :] += dot(high, pick_through) + dot(low, pick_through)

    @pl.when(step == steps - 1)
    def _():
        both = sums_ref[...].T
        square = (length, length)
        later = onehot(iota(square, 0) >= iota(square, 1))
        back = sum(dot(piece, later) for piece in split(both[:SLOTS], 3))
        dd_ref[...] = both[SLOTS:] / delta_ref[...] - rate_ref[...] * back


def final_part(
    x, dy, xs, ys, start, end, u, table, low, up, gb, gc, skip, delta, rate, writer, reader, first_group, grad_dtype
):
    length, lanes = x.shape
    steps = lanes // TILE
    local_groups = low.shape[0]
    per_group = steps // local_groups
    tile = lambda rows: pl.BlockSpec((rows, TILE), lambda i, f: (0, i))
    whole = lambda *shape: pl.BlockSpec(shape, lambda i, f: (0,) * len(shape))
    group = lambda rows, cols: pl.BlockSpec((None, rows, cols), lambda i, f: (i // per_group, 0, 0))
    proj = pl.BlockSpec((length, N), lambda i, f: (0, f[0] + i // per_group))
    shape = jax.ShapeDtypeStruct
    return pl.pallas_call(
        functools.partial(final_kernel, per_group, steps),
        grid_spec=pltpu.PrefetchScalarGridSpec(
            num_scalar_prefetch=1,
            grid=(steps,),
            in_specs=[
                tile(length),
                tile(length),
                tile(length),
                tile(length),
                tile(N),
                tile(N),
                tile(N),
                whole(2, length, 2 * SLOTS),
                group(length, length),
                group(length, length),
                proj,
                proj,
                group(length, N),
                group(length, N),
                tile(1),
                whole(SLOTS, length),
                whole(SLOTS, 1),
            ],
            out_specs=[
                tile(length),
                tile(length),
                pl.BlockSpec((length, N), lambda i, f: (0, i // per_group)),
                pl.BlockSpec((length, N), lambda i, f: (0, i // per_group)),
                whole(SLOTS, length),
            ],
            scratch_shapes=[
                pltpu.VMEM((length, 2 * SLOTS), F32),
                pltpu.VMEM((length, N), F32),
                pltpu.VMEM((length, N), F32),
            ],
        ),
        out_shape=[
            shape((length, lanes), BF16),
            shape((length, lanes), BF16),
            shape((length, local_groups * N), grad_dtype),
            shape((length, local_groups * N), grad_dtype),
            shape((SLOTS, length), F32),
        ],
        cost_estimate=pl.CostEstimate(
            flops=12 * length * lanes * length, transcendentals=0, bytes_accessed=16 * length * lanes
        ),
        name="final_part",
    )(
        first_group, x, dy, xs, ys, start, end, u, table, low, up, writer, reader, gb, gc, skip, delta, rate
    )


def tree_states(u, v, decay, parents, levels):
    segs = lax.axis_size("seg")
    lanes = u.shape[1]
    chunk = lanes // segs

    def spread_heads(state):
        parts = jnp.swapaxes(state.reshape(N, segs, chunk), 0, 1)
        return lax.all_to_all(parts, "seg", 0, 0)

    decay_all = lax.all_to_all(decay.reshape(segs, chunk), "seg", 0, 0)[:, None, :]
    u_all = spread_heads(u)
    v_all = spread_heads(v).astype(F32)
    safe = jnp.maximum(parents, 0)
    starts = jnp.zeros_like(u_all)
    for repeat in range(DEPTH - 1):
        ends = (decay_all * starts.astype(F32) + u_all.astype(F32)).astype(BF16)
        starts = jnp.where((levels == repeat + 1)[:, None, None], ends[safe], starts)
    link = (parents[None, :] == jnp.arange(segs)[:, None]).astype(F32)
    grad_end = jnp.zeros_like(v_all)
    for repeat in range(DEPTH - 1):
        lifted = decay_all * grad_end + v_all
        grad_end = sum(link[:, c, None, None] * lifted[c][None] for c in range(segs))

    def gather_heads(state):
        parts = lax.all_to_all(state, "seg", 0, 0)
        return jnp.swapaxes(parts, 0, 1).reshape(N, lanes)

    return gather_heads(starts), gather_heads(grad_end.astype(BF16))


def group_grads(gb, gc, members):
    shards_ = lax.axis_size("head")
    both = jnp.stack([gb, gc])
    length, width = gb.shape
    parts = both.reshape(2, shards_, length // shards_, width)
    parts = lax.all_to_all(parts, "head", 1, 1)
    if members > 1:
        parts = parts.reshape(2, shards_ // members, members, length // shards_, width).sum(2)
    parts = jnp.swapaxes(parts, 1, 2).reshape(2, length // shards_, -1)
    return parts.astype(BF16)


def chunk_of(place, k):
    return jnp.bitwise_xor(place[1], k)


def group_of(chunk, segs):
    return chunk * 2 // segs


def pack(ref, top, bottom, row, cols):
    ref[:N, cols] = top
    ref[N : 2 * N, cols] = bottom
    rows = iota((EXTRA, row.shape[1]), 0)
    high, mid, low = split(row, 3)
    tail = jnp.where(rows == 0, high.astype(F32), 0.0)
    tail = tail + jnp.where(rows == 1, mid.astype(F32), 0.0)
    ref[2 * N :, cols] = (tail + jnp.where(rows == 2, low.astype(F32), 0.0)).astype(BF16)


def tables(delta_ref, rate_ref):
    length = delta_ref.shape[1]
    square = (length, length)
    tri = onehot(iota(square, 0) >= iota(square, 1))
    eye = onehot(iota(square, 0) == iota(square, 1))
    pieces = split(delta_ref[...], 3)
    sums = sum(dot(tri, piece, NT) for piece in pieces)
    delta = sum(dot(eye, piece, NT) for piece in pieces)
    log = rate_ref[...] * sums
    grow = split(jnp.exp(log) * delta, 2)
    fall = split(jnp.exp(-log), 2)
    return jnp.concatenate(fall, axis=1), jnp.concatenate(grow, axis=1)


def spread_at(lane):
    shape = (2 * SLOTS, TILE)
    head = (lane + iota(shape, 1)) // P_SIZE
    return onehot((iota(shape, 0) % SLOTS) == head)


def states_kernel(far, segs, place, x_ref, dy_ref, *refs):
    count = segs // 2
    if far:
        delta_ref, rate_ref, b_ref, c_ref, *outs = refs
        *messages, xs_ref, ys_ref, table_ref, bt_ref, ct_ref = outs
    else:
        table_ref, b_ref, c_ref, *outs = refs
        *messages, xs_ref, ys_ref, bt_ref, ct_ref = outs
    step = pl.program_id(0)
    length, width = x_ref.shape

    @pl.when(step == 0)
    def _():
        if far:
            table_ref[0], table_ref[1] = tables(delta_ref, rate_ref)
        bt_ref[...] = b_ref[...].T
        ct_ref[...] = c_ref[...].T

    chunk = chunk_of(place, step + (count if far else 0))
    made = []
    for at in range(0, width, TILE):
        cols = slice(at, at + TILE)
        lanes = spread_at(chunk * width + at)
        fall = dot(table_ref[0], lanes)
        grow = dot(table_ref[1], lanes)
        xs, xs_low = split(x_ref[:, cols].astype(F32) * grow, 2)
        ys, ys_low = split(dy_ref[:, cols].astype(F32) * fall, 2)
        xs_ref[:, cols] = xs
        ys_ref[:, cols] = ys
        total = fall[length - 1 :]
        u = (dot(bt_ref[...], xs) + dot(bt_ref[...], xs_low)) * total
        v = dot(ct_ref[...], ys) + dot(ct_ref[...], ys_low)
        made.append((u.astype(BF16), v.astype(BF16), total, cols))
    for at, message in enumerate(messages):

        @pl.when(step == at)
        def _(message=message):
            for u, v, total, cols in made:
                pack(message, u, v, total, cols)


def half_specs(length, width, segs, far):
    first = segs // 2 if far else 0
    tile = lambda rows: pl.BlockSpec((rows, width), lambda i, f: (0, chunk_of(f, first + i)))
    turn = lambda rows: pl.BlockSpec((rows, width), lambda i, f: (0, i))
    whole = lambda *shape: pl.BlockSpec(shape, lambda i, f: (0,) * len(shape))
    proj = pl.BlockSpec(
        (length, N), lambda i, f: (0, 2 * f[0] + group_of(chunk_of(f, first), segs))
    )
    return tile, turn, whole, proj


def states_half(far, segs, place, x, dy, given, writer, reader):
    length, lanes = x.shape
    width = lanes // segs
    count = segs // 2
    tile, turn, whole, proj = half_specs(length, width, segs, far)
    shape = jax.ShapeDtypeStruct
    message = shape((2 * N + EXTRA, width), BF16)
    scaled = shape((length, lanes // 2), BF16)
    table = shape((2, length, 2 * SLOTS), BF16)
    return pl.pallas_call(
        functools.partial(states_kernel, far, segs),
        grid_spec=pltpu.PrefetchScalarGridSpec(
            num_scalar_prefetch=1,
            grid=(count,),
            in_specs=[tile(length), tile(length)]
            + [whole(*value.shape) for value in given]
            + [proj, proj],
            out_specs=[whole(*message.shape)] * count
            + [turn(length), turn(length)]
            + ([whole(*table.shape)] if far else []),
            scratch_shapes=[pltpu.VMEM((N, length), BF16)] * 2,
        ),
        out_shape=[message] * count + [scaled, scaled] + ([table] if far else []),
        cost_estimate=pl.CostEstimate(
            flops=4 * length * lanes * length, transcendentals=0, bytes_accessed=8 * length * lanes
        ),
        name="states_far" if far else "states_near",
    )(place, x, dy, *given, writer, reader)


def scores_kernel(count, _, xs_ref, ys_ref, b_ref, c_ref, low_ref, up_ref, gb_ref, gc_ref, acc_ref):
    step = pl.program_id(0)
    length = xs_ref.shape[0]
    square = (length, length)
    part = dot(ys_ref[...], xs_ref[...], NT)

    @pl.when(step == 0)
    def _():
        acc_ref[...] = part

    @pl.when(step > 0)
    def _():
        acc_ref[...] += part

    @pl.when(step == count - 1)
    def _():
        b, c = b_ref[...], c_ref[...]
        lower = iota(square, 0) >= iota(square, 1)
        upper = iota(square, 0) <= iota(square, 1)
        low_ref[...] = jnp.where(lower, dot(c, b, NT), 0.0).astype(BF16)
        up_ref[...] = jnp.where(upper, dot(b, c, NT), 0.0).astype(BF16)
        high, low = split(jnp.where(lower, acc_ref[...], 0.0), 2)
        gc_ref[...] = dot(high, b) + dot(low, b)
        gb_ref[...] = dot(high, c, ((0,), (0,))) + dot(low, c, ((0,), (0,)))


def scores_half(far, segs, place, xs, ys, writer, reader):
    length, lanes = xs.shape
    width = 2 * lanes // segs
    count = segs // 2
    _, turn, whole, proj = half_specs(length, width, segs, far)
    shape = jax.ShapeDtypeStruct
    return pl.pallas_call(
        functools.partial(scores_kernel, count),
        grid_spec=pltpu.PrefetchScalarGridSpec(
            num_scalar_prefetch=1,
            grid=(count,),
            in_specs=[turn(length), turn(length), proj, proj],
            out_specs=[whole(length, length)] * 2 + [whole(length, N)] * 2,
            scratch_shapes=[pltpu.VMEM((length, length), F32)],
        ),
        out_shape=[shape((length, length), BF16)] * 2 + [shape((length, N), F32)] * 2,
        cost_estimate=pl.CostEstimate(
            flops=2 * length * lanes * length, transcendentals=0, bytes_accessed=4 * length * lanes
        ),
        name="scores",
    )(place, xs, ys, writer, reader)


def tree_kernel(segs, place, parents, *refs):
    got, sent = refs[:segs], refs[segs : 2 * segs]
    all_ref, end_ref = refs[2 * segs :]
    width = all_ref.shape[2]
    cols = slice(0, width)
    for k in range(segs):
        all_ref[chunk_of(place, k)] = got[k][...]
    end_ref[...] = jnp.zeros_like(end_ref)

    def decay(seg):
        return jnp.sum(all_ref[seg, 2 * N :, :].astype(F32), axis=0, keepdims=True)

    for seg in range(segs):
        parent = parents[seg]
        near = jnp.maximum(parent, 0)
        above = jnp.where(parent >= 0, parents[near], -1)

        @pl.when(parent >= 0)
        def _():
            end_ref[near] += all_ref[seg, N : 2 * N, :].astype(F32)

        @pl.when(above >= 0)
        def _():
            end_ref[jnp.maximum(above, 0)] += decay(near) * all_ref[seg, N : 2 * N, :].astype(F32)

    for k in range(segs):
        seg = chunk_of(place, k)
        parent = parents[seg]
        near = jnp.maximum(parent, 0)
        above = jnp.where(parent >= 0, parents[near], -1)
        state = all_ref[near, :N, :].astype(F32)
        lifted = decay(near) * all_ref[jnp.maximum(above, 0), :N, :].astype(F32)
        start = jnp.where(parent >= 0, state, 0.0) + jnp.where(above >= 0, lifted, 0.0)
        start = start.astype(BF16)
        own = decay(seg)
        end = (own * end_ref[seg]).astype(BF16)
        held = start.astype(F32) + all_ref[seg, :N, :].astype(F32) / own
        last = jnp.sum(end.astype(F32) * held, axis=0, keepdims=True)
        pack(sent[k], start, end, last, cols)


def tree_chunk(segs, place, parents, messages):
    rows, width = messages[0].shape
    piece = 128
    block = pl.BlockSpec((rows, piece), lambda i, f, p: (0, i))
    return pl.pallas_call(
        functools.partial(tree_kernel, segs),
        grid_spec=pltpu.PrefetchScalarGridSpec(
            num_scalar_prefetch=2,
            grid=(width // piece,),
            in_specs=[block] * segs,
            out_specs=[block] * segs,
            scratch_shapes=[
                pltpu.VMEM((segs, rows, piece), BF16),
                pltpu.VMEM((segs, N, piece), F32),
            ],
        ),
        out_shape=[jax.ShapeDtypeStruct((rows, width), BF16)] * segs,
        cost_estimate=pl.CostEstimate(flops=10**7, transcendentals=0, bytes_accessed=10**7),
        name="tree",
    )(place, parents, *messages)


def outputs_kernel(far, segs, place, *refs):
    count = segs // 2
    messages, refs = refs[:count], refs[count:]
    x_ref, dy_ref, xs_ref, ys_ref, table_ref, low_ref, up_ref, b_ref, c_ref = refs[:9]
    gb_in, gc_in, skip_ref, refs = *refs[9:12], refs[12:]
    if far:
        sums_in, delta_ref, rate_ref, _, _, out_ref, dx_ref, grads_ref, dd_ref = refs[:9]
        *_, sums_ref, accb_ref, accc_ref, state_ref = refs
    else:
        out_ref, dx_ref, grads_ref, sums_ref, accb_ref, accc_ref, state_ref = refs
    step = pl.program_id(0)
    length, width = x_ref.shape
    for at, message in enumerate(messages):

        @pl.when(step == at)
        def _(message=message):
            state_ref[...] = message[...]

    @pl.when(step == 0)
    def _():
        accb_ref[...] = gb_in[...]
        accc_ref[...] = gc_in[...]
        sums_ref[...] = sums_in[...] if far else jnp.zeros_like(sums_ref)

    chunk = chunk_of(place, step + (count if far else 0))
    for at in range(0, width, TILE):
        cols = slice(at, at + TILE)
        lane = chunk * width + at
        lanes = spread_at(lane)
        fall = dot(table_ref[0], lanes)
        grow = dot(table_ref[1], lanes)
        xs, ys = xs_ref[:, cols], ys_ref[:, cols]
        start, end = state_ref[:N, cols], state_ref[N : 2 * N, cols]
        core = dot(low_ref[...], xs) + dot(c_ref[...], start)
        grad = dot(up_ref[...], ys) + dot(b_ref[...], end)
        skip = skip_ref[:, cols]
        out_ref[:, cols] = (fall * core + skip * x_ref[:, cols].astype(F32)).astype(BF16)
        dx_ref[:, cols] = (grow * grad + skip * dy_ref[:, cols].astype(F32)).astype(BF16)
        accc_ref[...] += dot(ys, start, NT)
        accb_ref[...] += dot(xs, end, NT)
        direct = xs.astype(F32) * grad
        through = ys.astype(F32) * core - direct
        shape = (TILE, 2 * SLOTS)
        column = iota(shape, 1)
        head = (lane + iota(shape, 0)) // P_SIZE
        pick_through = onehot(column == head)
        pick_direct = onehot(column == head + SLOTS)
        high, low = split(through, 2)
        dhigh, dlow = split(direct, 2)
        rows = dot(high, pick_through) + dot(low, pick_through)
        sums_ref[...] += rows + dot(dhigh, pick_direct) + dot(dlow, pick_direct)
        last = jnp.sum(state_ref[2 * N :, cols].astype(F32), axis=0, keepdims=True)
        at_last = jnp.where(iota((8, TILE), 0) == 7, last, 0.0)
        high, low = split(at_last, 2)
        sums_ref[length - 8 :, :] += dot(high, pick_through) + dot(low, pick_through)

    @pl.when(step == count - 1)
    def _():
        heads = grads_ref.shape[0]
        block = length // heads
        for k in range(heads):
            row = jnp.bitwise_xor(place[0], k) * block
            rows = pl.ds(pl.multiple_of(row, block), block)
            grads_ref[k, 0] = accb_ref[rows, :].astype(BF16)
            grads_ref[k, 1] = accc_ref[rows, :].astype(BF16)
        if far:
            both = sums_ref[...].T
            square = (length, length)
            later = onehot(iota(square, 0) >= iota(square, 1))
            back = sum(dot(piece, later) for piece in split(both[:SLOTS], 3))
            dd_ref[...] = both[SLOTS:] / delta_ref[...] - rate_ref[...] * back


def outputs_half(far, segs, heads, place, messages, x, dy, xs, ys, table, local, skip, writer, reader, earlier=()):
    length, lanes = x.shape
    width = lanes // segs
    count = segs // 2
    tile, turn, whole, proj = half_specs(length, width, segs, far)
    low, up, gb, gc = local
    shape = jax.ShapeDtypeStruct
    sums = shape((length, 2 * SLOTS), F32)
    full = shape((length, lanes), BF16)
    grads = shape((heads, 2, length // heads, N), BF16)
    any_ = pl.BlockSpec(memory_space=pl.ANY)
    in_specs = (
        [whole(2 * N + EXTRA, width)] * count
        + [tile(length), tile(length), turn(length), turn(length)]
        + [whole(*table.shape), whole(length, length), whole(length, length), proj, proj]
        + [whole(length, N), whole(length, N), tile(1)]
    )
    args = [*messages, x, dy, xs, ys, table, low, up, writer, reader, gb, gc, skip]
    out_specs = [tile(length), tile(length), whole(*grads.shape)]
    out_shape = [full, full, grads]
    scratch = [pltpu.VMEM((length, N), F32)] * 2 + [pltpu.VMEM((2 * N + EXTRA, width), BF16)]
    aliases = {}
    if far:
        sums_in, delta, rate, out, dx = earlier
        in_specs += [whole(*sums.shape), whole(*delta.shape), whole(*rate.shape), any_, any_]
        args += [sums_in, delta, rate, out, dx]
        out_specs.append(whole(*delta.shape))
        out_shape.append(shape(delta.shape, F32))
        scratch = [pltpu.VMEM(sums.shape, F32)] + scratch
        aliases = {len(args) - 1: 0, len(args): 1}
    else:
        out_specs.append(whole(*sums.shape))
        out_shape.append(sums)
    return pl.pallas_call(
        functools.partial(outputs_kernel, far, segs),
        grid_spec=pltpu.PrefetchScalarGridSpec(
            num_scalar_prefetch=1,
            grid=(count,),
            in_specs=in_specs,
            out_specs=out_specs,
            scratch_shapes=scratch,
        ),
        out_shape=out_shape,
        input_output_aliases=aliases,
        cost_estimate=pl.CostEstimate(
            flops=6 * length * lanes * length, transcendentals=0, bytes_accessed=8 * length * lanes
        ),
        name="outputs_far" if far else "outputs_near",
    )(place, *args)


def place_kernel(heads, segs, place, *refs):
    near, far, (gb_ref, gc_ref) = refs[:heads], refs[heads : 2 * heads], refs[2 * heads :]
    for k in range(heads):
        owner = jnp.bitwise_xor(place[0], k)
        for half, parts in enumerate((near, far)):
            group = 2 * owner + group_of(chunk_of(place, half * segs // 2), segs)
            cols = pl.ds(pl.multiple_of(group * N, N), N)
            gb_ref[:, cols] = parts[k][0]
            gc_ref[:, cols] = parts[k][1]


def place_grads(segs, place, near, far):
    heads = len(near)
    rows = near[0].shape[1]
    shape = jax.ShapeDtypeStruct((rows, 2 * heads * N), BF16)
    return pl.pallas_call(
        functools.partial(place_kernel, heads, segs),
        grid_spec=pltpu.PrefetchScalarGridSpec(
            num_scalar_prefetch=1,
            grid=(1,),
            in_specs=[pl.BlockSpec(near[0].shape, lambda i, f: (0, 0, 0))] * (2 * heads),
            out_specs=[pl.BlockSpec(shape.shape, lambda i, f: (0, 0))] * 2,
        ),
        out_shape=[shape] * 2,
        name="place_grads",
    )(place, *near, *far)


def swap(value, axis, k):
    size = lax.axis_size(axis)
    return lax.ppermute(value, axis, [(i, i ^ k) for i in range(size)])


def paired(inputs, deltas, rates, skips, writer, reader, grad_out, parents):
    segs = lax.axis_size("seg")
    heads = lax.axis_size("head")
    count = segs // 2
    place = jnp.stack([lax.axis_index("head"), lax.axis_index("seg")]).astype(jnp.int32)
    x, dy, b, c = inputs[0], grad_out[0], writer[0], reader[0]
    delta = deltas[0]
    *far, xs_far, ys_far, table = states_half(
        True, segs, place, x, dy, (delta, rates[None, :]), b, c
    )
    *near, xs_near, ys_near = states_half(False, segs, place, x, dy, (table,), b, c)
    got_far = [swap(far[k], "seg", count + k) for k in range(count)]
    got_near = [near[0]] + [swap(near[k], "seg", k) for k in range(1, count)]
    local_far = scores_half(True, segs, place, xs_far, ys_far, b, c)
    local_near = scores_half(False, segs, place, xs_near, ys_near, b, c)
    sent = tree_chunk(segs, place, parents, got_near + got_far)
    back_far = [swap(sent[k], "seg", k) for k in range(count, segs)]
    back_near = [sent[0]] + [swap(sent[k], "seg", k) for k in range(1, count)]
    skip = jnp.repeat(skips, P_SIZE)[None, :]
    out, dx, grads_near, sums = outputs_half(
        False, segs, heads, place, back_near, x, dy, xs_near, ys_near, table, local_near, skip, b, c
    )
    moved_near = [grads_near[0]] + [swap(grads_near[k], "head", k) for k in range(1, heads)]
    out, dx, grads_far, dd = outputs_half(
        True,
        segs,
        heads,
        place,
        back_far,
        x,
        dy,
        xs_far,
        ys_far,
        table,
        local_far,
        skip,
        b,
        c,
        (sums, delta, rates[:, None], out, dx),
    )
    moved_far = [grads_far[0]] + [swap(grads_far[k], "head", k) for k in range(1, heads)]
    gb, gc = place_grads(segs, place, moved_near, moved_far)
    return out[None], dx[None], dd[None], gb[None], gc[None]


def power_of_two(size):
    return size & (size - 1) == 0


def shards(inputs, deltas, rates, skips, writer, reader, grad_out, parents, levels):
    heads = deltas.shape[1]
    per_group_all = H // G
    local_groups = max(1, heads // per_group_all)
    members = max(1, per_group_all // heads)
    segs = lax.axis_size("seg")
    lanes = inputs.shape[2]
    even = power_of_two(segs) and power_of_two(lax.axis_size("head")) and segs >= 4
    if even and local_groups == 2 and heads == SLOTS and lanes // segs % TILE == 0:
        return paired(inputs, deltas, rates, skips, writer, reader, grad_out, parents)
    first_group = (lax.axis_index("head") * heads // per_group_all).astype(jnp.int32)[None]
    x, dy = inputs[0], grad_out[0]
    pad = SLOTS - heads
    delta = jnp.pad(deltas[0], ((0, pad), (0, 0)))
    rate = jnp.pad(rates, (0, pad))
    u, v, xs, ys, table, low, up, gb, gc = local_part(
        x, dy, delta, rate[None, :], writer[0], reader[0], first_group, local_groups
    )
    decay = jnp.repeat(jnp.exp(-rates * jnp.sum(deltas[0], axis=1)), P_SIZE)
    start, end = tree_states(u, v, decay, parents, levels)
    out, dx, gb, gc, dd = final_part(
        x,
        dy,
        xs,
        ys,
        start,
        end,
        u,
        table,
        low,
        up,
        gb,
        gc,
        jnp.repeat(skips, P_SIZE)[None, :],
        delta,
        rate[:, None],
        writer[0],
        reader[0],
        first_group,
        BF16 if members == 1 else F32,
    )
    grads = group_grads(gb, gc, members)
    return (out[None], dx[None], dd[None, :heads], grads[0][None], grads[1][None])


def solution(mesh):
    placed = (
        P("seg", None, "head"),
        P("seg", "head", None),
        P("head"),
        P("head"),
        P("seg", None, None),
        P("seg", None, None),
        P("seg", None, "head"),
        P(),
        P(),
    )
    return jax.shard_map(
        shards,
        mesh=mesh,
        in_specs=placed,
        out_specs=(
            P("seg", None, "head"),
            P("seg", None, "head"),
            P("seg", "head", None),
            P("seg", "head", None),
            P("seg", "head", None),
        ),
        check_vma=False,
    )
```

```python
import functools

import jax
import jax.numpy as jnp
from jax import lax
from jax.experimental import pallas as pl
from jax.experimental.pallas import tpu as pltpu
from jax.sharding import PartitionSpec as P


H = 256
P_SIZE = 64
N = 128
G = 8
DEPTH = 3
TILE = 256
SLOTS = 64
LANES = 128
EXTRA = 16
PIECES = 2

F32 = jnp.float32
BF16 = jnp.bfloat16


def dot(a, b, dims=((1,), (0,))):
    return lax.dot_general(a, b, (dims, ((), ())), preferred_element_type=F32)


NT = ((1,), (1,))


def split(value, parts):
    pieces = []
    for _ in range(parts):
        piece = value.astype(BF16)
        pieces.append(piece)
        value = value - piece.astype(F32)
    return pieces


def iota(shape, axis):
    return lax.broadcasted_iota(jnp.int32, shape, axis)


def onehot(cond):
    return jnp.where(cond, 1.0, 0.0).astype(BF16)


def spread(step):
    shape = (2 * SLOTS, TILE)
    head = step * (TILE // P_SIZE) + iota(shape, 1) // P_SIZE
    return onehot((iota(shape, 0) % SLOTS) == head)


def local_kernel(
    per_group,
    _,
    x_ref,
    dy_ref,
    delta_ref,
    rate_ref,
    b_ref,
    c_ref,
    u_ref,
    v_ref,
    xs_ref,
    ys_ref,
    table_ref,
    low_ref,
    up_ref,
    gb_ref,
    gc_ref,
    acc_ref,
):
    step = pl.program_id(0)
    length = x_ref.shape[0]
    square = (length, length)

    @pl.when(step == 0)
    def _():
        tri = onehot(iota(square, 0) >= iota(square, 1))
        eye = onehot(iota(square, 0) == iota(square, 1))
        pieces = split(delta_ref[...], 3)
        sums = sum(dot(tri, piece, NT) for piece in pieces)
        delta = sum(dot(eye, piece, NT) for piece in pieces)
        log = rate_ref[...] * sums
        grow = split(jnp.exp(log) * delta, 2)
        fall = split(jnp.exp(-log), 2)
        table_ref[0] = jnp.concatenate(fall, axis=1)
        table_ref[1] = jnp.concatenate(grow, axis=1)

    lanes = spread(step)
    fall = dot(table_ref[0], lanes)
    grow = dot(table_ref[1], lanes)
    xs, xs_low = split(x_ref[...].astype(F32) * grow, 2)
    ys, ys_low = split(dy_ref[...].astype(F32) * fall, 2)
    xs_ref[...] = xs
    ys_ref[...] = ys
    b, c = b_ref[...], c_ref[...]
    u = dot(b, xs, ((0,), (0,))) + dot(b, xs_low, ((0,), (0,)))
    v = dot(c, ys, ((0,), (0,))) + dot(c, ys_low, ((0,), (0,)))
    u_ref[...] = (u * fall[length - 1 :]).astype(BF16)
    v_ref[...] = v.astype(BF16)
    part = dot(ys, xs, NT)
    inner = step % per_group

    @pl.when(inner == 0)
    def _():
        acc_ref[...] = part

    @pl.when(inner > 0)
    def _():
        acc_ref[...] += part

    @pl.when(inner == per_group - 1)
    def _():
        lower = iota(square, 0) >= iota(square, 1)
        upper = iota(square, 0) <= iota(square, 1)
        low_ref[...] = jnp.where(lower, dot(c, b, NT), 0.0).astype(BF16)
        up_ref[...] = jnp.where(upper, dot(b, c, NT), 0.0).astype(BF16)
        high, low = split(jnp.where(lower, acc_ref[...], 0.0), 2)
        gc_ref[...] = dot(high, b) + dot(low, b)
        gb_ref[...] = dot(high, c, ((0,), (0,))) + dot(low, c, ((0,), (0,)))


def local_part(x, dy, delta, rate, writer, reader, first_group, local_groups):
    length, lanes = x.shape
    steps = lanes // TILE
    per_group = steps // local_groups
    tile = lambda rows: pl.BlockSpec((rows, TILE), lambda i, f: (0, i))
    whole = lambda *shape: pl.BlockSpec(shape, lambda i, f: (0,) * len(shape))
    group = lambda rows, cols: pl.BlockSpec((None, rows, cols), lambda i, f: (i // per_group, 0, 0))
    proj = pl.BlockSpec((length, N), lambda i, f: (0, f[0] + i // per_group))
    shape = jax.ShapeDtypeStruct
    return pl.pallas_call(
        functools.partial(local_kernel, per_group),
        grid_spec=pltpu.PrefetchScalarGridSpec(
            num_scalar_prefetch=1,
            grid=(steps,),
            in_specs=[
                tile(length),
                tile(length),
                whole(SLOTS, length),
                whole(1, SLOTS),
                proj,
                proj,
            ],
            out_specs=[
                tile(N),
                tile(N),
                tile(length),
                tile(length),
                whole(2, length, 2 * SLOTS),
                group(length, length),
                group(length, length),
                group(length, N),
                group(length, N),
            ],
            scratch_shapes=[pltpu.VMEM((length, length), F32)],
        ),
        out_shape=[
            shape((N, lanes), BF16),
            shape((N, lanes), BF16),
            shape((length, lanes), BF16),
            shape((length, lanes), BF16),
            shape((2, length, 2 * SLOTS), BF16),
            shape((local_groups, length, length), BF16),
            shape((local_groups, length, length), BF16),
            shape((local_groups, length, N), F32),
            shape((local_groups, length, N), F32),
        ],
        cost_estimate=pl.CostEstimate(
            flops=8 * length * lanes * length, transcendentals=0, bytes_accessed=12 * length * lanes
        ),
        name="local_part",
    )(first_group, x, dy, delta, rate, writer, reader)


def final_kernel(
    per_group,
    steps,
    _,
    x_ref,
    dy_ref,
    xs_ref,
    ys_ref,
    start_ref,
    end_ref,
    u_ref,
    table_ref,
    low_ref,
    up_ref,
    b_ref,
    c_ref,
    gb_in,
    gc_in,
    skip_ref,
    delta_ref,
    rate_ref,
    out_ref,
    dx_ref,
    gb_ref,
    gc_ref,
    dd_ref,
    sums_ref,
    accb_ref,
    accc_ref,
):
    step = pl.program_id(0)
    length = x_ref.shape[0]
    lanes = spread(step)
    fall = dot(table_ref[0], lanes)
    grow = dot(table_ref[1], lanes)
    xs, ys, start = xs_ref[...], ys_ref[...], start_ref[...]
    total = fall[length - 1 :]
    end = end_ref[...].astype(F32) * total
    end_high, end_low = split(end, 2)
    core = dot(low_ref[...], xs) + dot(c_ref[...], start)
    grad = dot(up_ref[...], ys) + dot(b_ref[...], end_high) + dot(b_ref[...], end_low)
    skip = skip_ref[...]
    out_ref[...] = (fall * core + skip * x_ref[...].astype(F32)).astype(out_ref.dtype)
    dx_ref[...] = (grow * grad + skip * dy_ref[...].astype(F32)).astype(dx_ref.dtype)

    inner = step % per_group

    @pl.when(inner == 0)
    def _():
        accb_ref[...] = gb_in[...]
        accc_ref[...] = gc_in[...]

    accc_ref[...] += dot(ys, start, NT)
    accb_ref[...] += dot(xs, end_high, NT) + dot(xs, end_low, NT)

    @pl.when(inner == per_group - 1)
    def _():
        gb_ref[...] = accb_ref[...].astype(gb_ref.dtype)
        gc_ref[...] = accc_ref[...].astype(gc_ref.dtype)

    direct = xs.astype(F32) * grad
    through = ys.astype(F32) * core - direct
    shape = (TILE, 2 * SLOTS)
    column = iota(shape, 1)
    head = step * (TILE // P_SIZE) + iota(shape, 0) // P_SIZE
    pick_through = onehot(column == head)
    pick_direct = onehot(column == head + SLOTS)
    high, low = split(through, 2)
    dhigh, dlow = split(direct, 2)
    rows = dot(high, pick_through) + dot(low, pick_through)
    rows = rows + dot(dhigh, pick_direct) + dot(dlow, pick_direct)

    @pl.when(step == 0)
    def _():
        sums_ref[...] = rows

    @pl.when(step > 0)
    def _():
        sums_ref[...] += rows

    held = u_ref[...].astype(F32) / total + start.astype(F32)
    last = jnp.sum(end * held, axis=0, keepdims=True)
    at_last = jnp.where(iota((8, TILE), 0) == 7, last, 0.0)
    high, low = split(at_last, 2)
    sums_ref[length - 8 :, :] += dot(high, pick_through) + dot(low, pick_through)

    @pl.when(step == steps - 1)
    def _():
        both = sums_ref[...].T
        square = (length, length)
        later = onehot(iota(square, 0) >= iota(square, 1))
        back = sum(dot(piece, later) for piece in split(both[:SLOTS], 3))
        dd_ref[...] = both[SLOTS:] / delta_ref[...] - rate_ref[...] * back


def final_part(
    x, dy, xs, ys, start, end, u, table, low, up, gb, gc, skip, delta, rate, writer, reader, first_group, grad_dtype
):
    length, lanes = x.shape
    steps = lanes // TILE
    local_groups = low.shape[0]
    per_group = steps // local_groups
    tile = lambda rows: pl.BlockSpec((rows, TILE), lambda i, f: (0, i))
    whole = lambda *shape: pl.BlockSpec(shape, lambda i, f: (0,) * len(shape))
    group = lambda rows, cols: pl.BlockSpec((None, rows, cols), lambda i, f: (i // per_group, 0, 0))
    proj = pl.BlockSpec((length, N), lambda i, f: (0, f[0] + i // per_group))
    shape = jax.ShapeDtypeStruct
    return pl.pallas_call(
        functools.partial(final_kernel, per_group, steps),
        grid_spec=pltpu.PrefetchScalarGridSpec(
            num_scalar_prefetch=1,
            grid=(steps,),
            in_specs=[
                tile(length),
                tile(length),
                tile(length),
                tile(length),
                tile(N),
                tile(N),
                tile(N),
                whole(2, length, 2 * SLOTS),
                group(length, length),
                group(length, length),
                proj,
                proj,
                group(length, N),
                group(length, N),
                tile(1),
                whole(SLOTS, length),
                whole(SLOTS, 1),
            ],
            out_specs=[
                tile(length),
                tile(length),
                pl.BlockSpec((length, N), lambda i, f: (0, i // per_group)),
                pl.BlockSpec((length, N), lambda i, f: (0, i // per_group)),
                whole(SLOTS, length),
            ],
            scratch_shapes=[
                pltpu.VMEM((length, 2 * SLOTS), F32),
                pltpu.VMEM((length, N), F32),
                pltpu.VMEM((length, N), F32),
            ],
        ),
        out_shape=[
            shape((length, lanes), BF16),
            shape((length, lanes), BF16),
            shape((length, local_groups * N), grad_dtype),
            shape((length, local_groups * N), grad_dtype),
            shape((SLOTS, length), F32),
        ],
        cost_estimate=pl.CostEstimate(
            flops=12 * length * lanes * length, transcendentals=0, bytes_accessed=16 * length * lanes
        ),
        name="final_part",
    )(
        first_group, x, dy, xs, ys, start, end, u, table, low, up, writer, reader, gb, gc, skip, delta, rate
    )


def tree_states(u, v, decay, parents, levels):
    segs = lax.axis_size("seg")
    lanes = u.shape[1]
    chunk = lanes // segs

    def spread_heads(state):
        parts = jnp.swapaxes(state.reshape(N, segs, chunk), 0, 1)
        return lax.all_to_all(parts, "seg", 0, 0)

    decay_all = lax.all_to_all(decay.reshape(segs, chunk), "seg", 0, 0)[:, None, :]
    u_all = spread_heads(u)
    v_all = spread_heads(v).astype(F32)
    safe = jnp.maximum(parents, 0)
    starts = jnp.zeros_like(u_all)
    for repeat in range(DEPTH - 1):
        ends = (decay_all * starts.astype(F32) + u_all.astype(F32)).astype(BF16)
        starts = jnp.where((levels == repeat + 1)[:, None, None], ends[safe], starts)
    link = (parents[None, :] == jnp.arange(segs)[:, None]).astype(F32)
    grad_end = jnp.zeros_like(v_all)
    for _ in range(DEPTH - 1):
        lifted = decay_all * grad_end + v_all
        grad_end = sum(link[:, c, None, None] * lifted[c][None] for c in range(segs))

    def gather_heads(state):
        parts = lax.all_to_all(state, "seg", 0, 0)
        return jnp.swapaxes(parts, 0, 1).reshape(N, lanes)

    return gather_heads(starts), gather_heads(grad_end.astype(BF16))


def group_grads(gb, gc, members):
    shards_ = lax.axis_size("head")
    both = jnp.stack([gb, gc])
    length, width = gb.shape
    parts = both.reshape(2, shards_, length // shards_, width)
    parts = lax.all_to_all(parts, "head", 1, 1)
    if members > 1:
        parts = parts.reshape(2, shards_ // members, members, length // shards_, width).sum(2)
    parts = jnp.swapaxes(parts, 1, 2).reshape(2, length // shards_, -1)
    return parts.astype(BF16)


def chunk_of(place, k):
    return jnp.bitwise_xor(place[1], k)


def group_of(chunk, segs):
    return chunk * 2 // segs


def message_rows(width):
    return 2 * N * (width // LANES // PIECES) + EXTRA


def pack_states(ref, block, top, bottom):
    row = 2 * N * block
    ref[row : row + N, :] = top
    ref[row + N : row + 2 * N, :] = bottom


def tail_rows(rows_of):
    rows = iota((EXTRA, LANES), 0)
    tail = jnp.zeros((EXTRA, LANES), F32)
    for block, row in rows_of:
        for piece, value in enumerate(split(row, 3)):
            tail = tail + jnp.where(rows == 3 * block + piece, value.astype(F32), 0.0)
    return tail


def tail_row(tail, block):
    rows = iota((EXTRA, LANES), 0)
    own = (rows >= 3 * block) & (rows < 3 * block + 3)
    return jnp.sum(jnp.where(own, tail.astype(F32), 0.0), axis=0, keepdims=True)


def tables(delta_ref, rate_ref):
    length = delta_ref.shape[1]
    square = (length, length)
    tri = onehot(iota(square, 0) >= iota(square, 1))
    eye = onehot(iota(square, 0) == iota(square, 1))
    pieces = split(delta_ref[...], 3)
    sums = sum(dot(tri, piece, NT) for piece in pieces)
    delta = sum(dot(eye, piece, NT) for piece in pieces)
    log = rate_ref[...] * sums
    grow = split(jnp.exp(log) * delta, 2)
    fall = split(jnp.exp(-log), 2)
    return jnp.concatenate(fall, axis=1), jnp.concatenate(grow, axis=1)


def spread_at(lane):
    shape = (2 * SLOTS, TILE)
    head = (lane + iota(shape, 1)) // P_SIZE
    return onehot((iota(shape, 0) % SLOTS) == head)


def states_kernel(first, lead, place, x_ref, dy_ref, *refs):
    if lead:
        delta_ref, rate_ref, b_ref, c_ref, *outs = refs
        *messages, xs_ref, ys_ref, table_ref, bt_ref, ct_ref = outs
    else:
        table_ref, b_ref, c_ref, *outs = refs
        *messages, xs_ref, ys_ref, bt_ref, ct_ref = outs
    step = pl.program_id(0)
    length, width = x_ref.shape

    @pl.when(step == 0)
    def _():
        if lead:
            table_ref[0], table_ref[1] = tables(delta_ref, rate_ref)
        bt_ref[...] = b_ref[...].T
        ct_ref[...] = c_ref[...].T

    chunk = chunk_of(place, step + first)
    made = []
    for at in range(0, width, TILE):
        cols = slice(at, at + TILE)
        lanes = spread_at(chunk * width + at)
        fall = dot(table_ref[0], lanes)
        grow = dot(table_ref[1], lanes)
        xs, xs_low = split(x_ref[:, cols].astype(F32) * grow, 2)
        ys, ys_low = split(dy_ref[:, cols].astype(F32) * fall, 2)
        xs_ref[:, cols] = xs
        ys_ref[:, cols] = ys
        total = fall[length - 1 :]
        u = (dot(bt_ref[...], xs) + dot(bt_ref[...], xs_low)) * total
        v = dot(ct_ref[...], ys) + dot(ct_ref[...], ys_low)
        for part in range(0, TILE, LANES):
            lane = slice(part, part + LANES)
            made.append((u[:, lane].astype(BF16), v[:, lane].astype(BF16), total[:, lane]))
    for at, message in enumerate(messages):

        @pl.when(step == at // PIECES)
        def _(message=message, piece=at % PIECES):
            blocks = len(made) // PIECES
            held = made[piece * blocks : (piece + 1) * blocks]
            for block, (u, v, _) in enumerate(held):
                pack_states(message, block, u, v)
            tail = tail_rows([(block, row) for block, (_, _, row) in enumerate(held)])
            message[message.shape[0] - EXTRA :, :] = tail.astype(BF16)


def part_specs(length, width, segs, first):
    tile = lambda rows: pl.BlockSpec((rows, width), lambda i, f: (0, chunk_of(f, first + i)))
    turn = lambda rows: pl.BlockSpec((rows, width), lambda i, f: (0, i))
    whole = lambda *shape: pl.BlockSpec(shape, lambda i, f: (0,) * len(shape))
    proj = pl.BlockSpec(
        (length, N), lambda i, f: (0, 2 * f[0] + group_of(chunk_of(f, first), segs))
    )
    return tile, turn, whole, proj


def states_part(first, count, segs, place, x, dy, given, writer, reader):
    length, lanes = x.shape
    width = lanes // segs
    lead = len(given) == 2
    tile, turn, whole, proj = part_specs(length, width, segs, first)
    shape = jax.ShapeDtypeStruct
    message = shape((message_rows(width), LANES), BF16)
    scaled = shape((length, count * width), BF16)
    table = shape((2, length, 2 * SLOTS), BF16)
    return pl.pallas_call(
        functools.partial(states_kernel, first, lead),
        grid_spec=pltpu.PrefetchScalarGridSpec(
            num_scalar_prefetch=1,
            grid=(count,),
            in_specs=[tile(length), tile(length)]
            + [whole(*value.shape) for value in given]
            + [proj, proj],
            out_specs=[whole(*message.shape)] * (count * PIECES)
            + [turn(length), turn(length)]
            + ([whole(*table.shape)] if lead else []),
            scratch_shapes=[pltpu.VMEM((N, length), BF16)] * 2,
        ),
        out_shape=[message] * (count * PIECES) + [scaled, scaled] + ([table] if lead else []),
        cost_estimate=pl.CostEstimate(
            flops=8 * length * count * width * length,
            transcendentals=0,
            bytes_accessed=16 * length * count * width,
        ),
    )(place, x, dy, *given, writer, reader)


def scores_kernel(count, pairs, _, *refs):
    scaled, (b_ref, c_ref) = refs[: 2 * pairs], refs[2 * pairs : 2 * pairs + 2]
    low_ref, up_ref, gb_ref, gc_ref, acc_ref = refs[2 * pairs + 2 :]
    step = pl.program_id(0)
    length = b_ref.shape[0]
    square = (length, length)
    part = sum(dot(scaled[2 * i + 1][...], scaled[2 * i][...], NT) for i in range(pairs))

    @pl.when(step == 0)
    def _():
        acc_ref[...] = part

    @pl.when(step > 0)
    def _():
        acc_ref[...] += part

    @pl.when(step == count - 1)
    def _():
        b, c = b_ref[...], c_ref[...]
        lower = iota(square, 0) >= iota(square, 1)
        upper = iota(square, 0) <= iota(square, 1)
        low_ref[...] = jnp.where(lower, dot(c, b, NT), 0.0).astype(BF16)
        up_ref[...] = jnp.where(upper, dot(b, c, NT), 0.0).astype(BF16)
        high, low = split(jnp.where(lower, acc_ref[...], 0.0), 2)
        gc_ref[...] = dot(high, b) + dot(low, b)
        gb_ref[...] = dot(high, c, ((0,), (0,))) + dot(low, c, ((0,), (0,)))


def scores_part(first, segs, width, place, scaled, writer, reader):
    length, lanes = scaled[0].shape
    count = lanes // width
    _, turn, whole, proj = part_specs(length, width, segs, first)
    shape = jax.ShapeDtypeStruct
    return pl.pallas_call(
        functools.partial(scores_kernel, count, len(scaled) // 2),
        grid_spec=pltpu.PrefetchScalarGridSpec(
            num_scalar_prefetch=1,
            grid=(count,),
            in_specs=[turn(length)] * len(scaled) + [proj, proj],
            out_specs=[whole(length, length)] * 2 + [whole(length, N)] * 2,
            scratch_shapes=[pltpu.VMEM((length, length), F32)],
        ),
        out_shape=[shape((length, length), BF16)] * 2 + [shape((length, N), F32)] * 2,
        cost_estimate=pl.CostEstimate(
            flops=4 * length * lanes * length, transcendentals=0, bytes_accessed=8 * length * lanes
        ),
    )(place, *scaled, writer, reader)


def tree_kernel(segs, place, parents, *refs):
    got, tails = refs[:segs], refs[segs : 2 * segs]
    sent = refs[2 * segs : 3 * segs]
    all_ref, end_ref, decay_ref, tail_ref = refs[3 * segs :]
    block = pl.program_id(0)
    for k in range(segs):
        seg = chunk_of(place, k)
        all_ref[seg] = got[k][...]
        decay_ref[seg] = tail_row(tails[k][...], block)
    end_ref[...] = jnp.zeros_like(end_ref)

    for seg in range(segs):
        parent = parents[seg]
        near = jnp.maximum(parent, 0)
        above = jnp.where(parent >= 0, parents[near], -1)

        @pl.when(parent >= 0)
        def _():
            end_ref[near] += all_ref[seg, N:, :].astype(F32)

        @pl.when(above >= 0)
        def _():
            end_ref[jnp.maximum(above, 0)] += decay_ref[near] * all_ref[seg, N:, :].astype(F32)

    rows = iota((EXTRA, LANES), 0)
    for k in range(segs):
        seg = chunk_of(place, k)
        parent = parents[seg]
        near = jnp.maximum(parent, 0)
        above = jnp.where(parent >= 0, parents[near], -1)
        state = all_ref[near, :N, :].astype(F32)
        lifted = decay_ref[near] * all_ref[jnp.maximum(above, 0), :N, :].astype(F32)
        start = jnp.where(parent >= 0, state, 0.0) + jnp.where(above >= 0, lifted, 0.0)
        start = start.astype(BF16)
        own = decay_ref[seg]
        end = (own * end_ref[seg]).astype(BF16)
        held = start.astype(F32) + all_ref[seg, :N, :].astype(F32) / own
        last = jnp.sum(end.astype(F32) * held, axis=0, keepdims=True)
        at = pl.multiple_of(block * 2 * N, 2 * N)
        sent[k][pl.ds(at, N), :] = start
        sent[k][pl.ds(pl.multiple_of(at + N, N), N), :] = end
        tail = tail_rows([(block, last)])
        tail_ref[k] = jnp.where(block == 0, tail, tail_ref[k] + tail)

    @pl.when(block == pl.num_programs(0) - 1)
    def _():
        for k in range(segs):
            sent[k][sent[k].shape[0] - EXTRA :, :] = tail_ref[k].astype(BF16)


def tree_chunk(segs, place, parents, messages):
    rows, _ = messages[0].shape
    blocks = (rows - EXTRA) // (2 * N)
    state = pl.BlockSpec((2 * N, LANES), lambda i, f, p: (i, 0))
    tail = pl.BlockSpec((EXTRA, LANES), lambda i, f, p: (2 * N * blocks // EXTRA, 0))
    return pl.pallas_call(
        functools.partial(tree_kernel, segs),
        grid_spec=pltpu.PrefetchScalarGridSpec(
            num_scalar_prefetch=2,
            grid=(blocks,),
            in_specs=[state] * segs + [tail] * segs,
            out_specs=[pl.BlockSpec((rows, LANES), lambda i, f, p: (0, 0))] * segs,
            scratch_shapes=[
                pltpu.VMEM((segs, 2 * N, LANES), BF16),
                pltpu.VMEM((segs, N, LANES), F32),
                pltpu.VMEM((segs, 1, LANES), F32),
                pltpu.VMEM((segs, EXTRA, LANES), F32),
            ],
        ),
        out_shape=[jax.ShapeDtypeStruct((rows, LANES), BF16)] * segs,
        cost_estimate=pl.CostEstimate(flops=10**7, transcendentals=0, bytes_accessed=10**7),
        name="tree",
    )(place, parents, *messages, *messages)


def unpack(messages, state_ref, last_ref):
    blocks = state_ref.shape[1] // LANES // PIECES
    for piece, message in enumerate(messages):
        tail = message[2 * N * blocks :, :]
        for block in range(blocks):
            lane = (piece * blocks + block) * LANES
            cols = slice(lane, lane + LANES)
            state_ref[:, cols] = message[2 * N * block : 2 * N * (block + 1), :]
            if last_ref is not None:
                last_ref[:, cols] = tail_row(tail, block)


def hand_out(place, outs, accb_ref, accc_ref):
    block = accb_ref.shape[0] // len(outs)
    for k, out in enumerate(outs):
        row = jnp.bitwise_xor(place[0], k) * block
        rows = pl.ds(pl.multiple_of(row, block), block)
        out[0] = accb_ref[rows, :].astype(BF16)
        out[1] = accc_ref[rows, :].astype(BF16)


def grads_kernel(count, whole, place, *refs):
    messages, refs = refs[: count * PIECES], refs[count * PIECES :]
    xs_ref, ys_ref, gb_in, gc_in, *outs, accb_ref, accc_ref, state_ref = refs
    step = pl.program_id(0)

    @pl.when(step == 0)
    def _():
        accb_ref[...] = gb_in[...]
        accc_ref[...] = gc_in[...]

    for at in range(count):

        @pl.when(step == at)
        def _(parts=messages[at * PIECES : (at + 1) * PIECES]):
            unpack(parts, state_ref, None)

    accc_ref[...] += dot(ys_ref[...], state_ref[:N, :], NT)
    accb_ref[...] += dot(xs_ref[...], state_ref[N:, :], NT)

    @pl.when(step == count - 1)
    def _():
        if whole:
            outs[0][...] = accb_ref[...]
            outs[1][...] = accc_ref[...]
        else:
            hand_out(place, outs, accb_ref, accc_ref)


def grads_part(first, segs, width, heads, place, messages, xs, ys, gb, gc):
    length, lanes = xs.shape
    count = lanes // width
    _, turn, whole, _ = part_specs(length, width, segs, first)
    block = jax.ShapeDtypeStruct((2, length // max(heads, 1), N), BF16)
    total = jax.ShapeDtypeStruct((length, N), F32)
    outs = [block] * heads if heads else [total, total]
    return pl.pallas_call(
        functools.partial(grads_kernel, count, not heads),
        grid_spec=pltpu.PrefetchScalarGridSpec(
            num_scalar_prefetch=1,
            grid=(count,),
            in_specs=[whole(*messages[0].shape)] * len(messages)
            + [turn(length)] * 2
            + [whole(length, N)] * 2,
            out_specs=[whole(*out.shape) for out in outs],
            scratch_shapes=[pltpu.VMEM((length, N), F32)] * 2 + [pltpu.VMEM((2 * N, width), BF16)],
        ),
        out_shape=outs,
        cost_estimate=pl.CostEstimate(
            flops=4 * length * count * width * N,
            transcendentals=0,
            bytes_accessed=8 * length * count * width,
        ),
    )(place, *messages, xs, ys, gb, gc)


def outputs_kernel(first, count, earlier, final, place, *refs):
    messages, refs = refs[: count * PIECES], refs[count * PIECES :]
    x_ref, dy_ref, xs_ref, ys_ref, table_ref, low_ref, up_ref, b_ref, c_ref, skip_ref = refs[:10]
    refs = refs[10:]
    if earlier:
        sums_in, _, _, *refs = refs
    if final:
        delta_ref, rate_ref, gb_in, gc_in, out_ref, dx_ref, dd_ref, *refs = refs
        *outs, accb_ref, accc_ref, sums_ref, state_ref, last_ref = refs
    else:
        out_ref, dx_ref, sums_ref, state_ref, last_ref = refs
    step = pl.program_id(0)
    length, width = x_ref.shape
    for at in range(count):

        @pl.when(step == at)
        def _(parts=messages[at * PIECES : (at + 1) * PIECES]):
            unpack(parts, state_ref, last_ref)

    @pl.when(step == 0)
    def _():
        if final:
            accb_ref[...] = gb_in[...]
            accc_ref[...] = gc_in[...]
        sums_ref[...] = sums_in[...] if earlier else jnp.zeros_like(sums_ref)

    chunk = chunk_of(place, step + first)
    for at in range(0, width, TILE):
        cols = slice(at, at + TILE)
        lane = chunk * width + at
        lanes = spread_at(lane)
        fall = dot(table_ref[0], lanes)
        grow = dot(table_ref[1], lanes)
        xs, ys = xs_ref[:, cols], ys_ref[:, cols]
        start, end = state_ref[:N, cols], state_ref[N:, cols]
        core = dot(low_ref[...], xs) + dot(c_ref[...], start)
        grad = dot(up_ref[...], ys) + dot(b_ref[...], end)
        skip = skip_ref[:, cols]
        out_ref[:, cols] = (fall * core + skip * x_ref[:, cols].astype(F32)).astype(BF16)
        dx_ref[:, cols] = (grow * grad + skip * dy_ref[:, cols].astype(F32)).astype(BF16)
        if final:
            accc_ref[...] += dot(ys, start, NT)
            accb_ref[...] += dot(xs, end, NT)
        direct = xs.astype(F32) * grad
        through = ys.astype(F32) * core - direct
        shape = (TILE, 2 * SLOTS)
        column = iota(shape, 1)
        head = (lane + iota(shape, 0)) // P_SIZE
        pick_through = onehot(column == head)
        pick_direct = onehot(column == head + SLOTS)
        high, low = split(through, 2)
        dhigh, dlow = split(direct, 2)
        rows = dot(high, pick_through) + dot(low, pick_through)
        sums_ref[...] += rows + dot(dhigh, pick_direct) + dot(dlow, pick_direct)
        at_last = jnp.where(iota((8, TILE), 0) == 7, last_ref[:, cols], 0.0)
        high, low = split(at_last, 2)
        sums_ref[length - 8 :, :] += dot(high, pick_through) + dot(low, pick_through)

    if final:

        @pl.when(step == count - 1)
        def _():
            hand_out(place, outs, accb_ref, accc_ref)
            both = sums_ref[...].T
            square = (length, length)
            later = onehot(iota(square, 0) >= iota(square, 1))
            back = sum(dot(piece, later) for piece in split(both[:SLOTS], 3))
            dd_ref[...] = both[SLOTS:] / delta_ref[...] - rate_ref[...] * back


def outputs_part(first, segs, place, messages, x, dy, xs, ys, table, low, up, skip, writer, reader, earlier=(), final=(), heads=0):
    length, lanes = x.shape
    width = lanes // segs
    count = len(messages) // PIECES
    tile, turn, whole, proj = part_specs(length, width, segs, first)
    shape = jax.ShapeDtypeStruct
    sums = shape((length, 2 * SLOTS), F32)
    full = shape((length, lanes), BF16)
    any_ = pl.BlockSpec(memory_space=pl.ANY)
    in_specs = (
        [whole(*messages[0].shape)] * len(messages)
        + [tile(length), tile(length), turn(length), turn(length)]
        + [whole(*table.shape), whole(length, length), whole(length, length), proj, proj]
        + [tile(1)]
    )
    args = [*messages, x, dy, xs, ys, table, low, up, writer, reader, skip]
    aliases = {}
    if earlier:
        in_specs += [whole(*sums.shape), any_, any_]
        args += list(earlier)
        aliases = {len(args) - 1: 0, len(args): 1}
    in_specs += [whole(*value.shape) for value in final]
    args += list(final)
    scratch = [pltpu.VMEM((2 * N, width), BF16), pltpu.VMEM((1, width), F32)]
    out_specs, out_shape = [tile(length), tile(length)], [full, full]
    if final:
        delta = final[0]
        out_specs.append(whole(*delta.shape))
        out_shape.append(shape(delta.shape, F32))
        block = shape((2, length // heads, N), BF16)
        out_specs += [whole(*block.shape)] * heads
        out_shape += [block] * heads
        scratch = [pltpu.VMEM((length, N), F32)] * 2 + [pltpu.VMEM(sums.shape, F32)] + scratch
    else:
        out_specs.append(whole(*sums.shape))
        out_shape.append(sums)
    return pl.pallas_call(
        functools.partial(outputs_kernel, first, count, bool(earlier), bool(final)),
        grid_spec=pltpu.PrefetchScalarGridSpec(
            num_scalar_prefetch=1,
            grid=(count,),
            in_specs=in_specs,
            out_specs=out_specs,
            scratch_shapes=scratch,
        ),
        out_shape=out_shape,
        input_output_aliases=aliases,
        cost_estimate=pl.CostEstimate(
            flops=12 * length * count * width * length,
            transcendentals=0,
            bytes_accessed=16 * length * count * width,
        ),
    )(place, *args)


def place_kernel(heads, segs, place, *refs):
    near, far, (gb_ref, gc_ref) = refs[:heads], refs[heads : 2 * heads], refs[2 * heads :]
    for k in range(heads):
        owner = jnp.bitwise_xor(place[0], k)
        for half, parts in enumerate((near, far)):
            group = 2 * owner + group_of(chunk_of(place, half * segs // 2), segs)
            cols = pl.ds(pl.multiple_of(group * N, N), N)
            gb_ref[:, cols] = parts[k][0]
            gc_ref[:, cols] = parts[k][1]


def place_grads(segs, place, near, far):
    heads = len(near)
    rows = near[0].shape[1]
    shape = jax.ShapeDtypeStruct((rows, 2 * heads * N), BF16)
    return pl.pallas_call(
        functools.partial(place_kernel, heads, segs),
        grid_spec=pltpu.PrefetchScalarGridSpec(
            num_scalar_prefetch=1,
            grid=(1,),
            in_specs=[pl.BlockSpec(near[0].shape, lambda i, f: (0, 0, 0))] * (2 * heads),
            out_specs=[pl.BlockSpec(shape.shape, lambda i, f: (0, 0))] * 2,
        ),
        out_shape=[shape] * 2,
        name="place_grads",
    )(place, *near, *far)


def swap(value, axis, k):
    size = lax.axis_size(axis)
    return lax.ppermute(value, axis, [(i, i ^ k) for i in range(size)])


def paired(inputs, deltas, rates, skips, writer, reader, grad_out, parents):
    segs = lax.axis_size("seg")
    heads = lax.axis_size("head")
    mid, late = segs // 2, 3 * segs // 4
    near_ks, mid_ks, late_ks = range(mid), range(mid, late), range(late, segs)
    place = jnp.stack([lax.axis_index("head"), lax.axis_index("seg")]).astype(jnp.int32)
    x, dy, b, c = inputs[0], grad_out[0], writer[0], reader[0]
    width = x.shape[1] // segs
    delta = deltas[0]
    own, got, back = {}, {}, {}

    def keep(ks, messages):
        for at, message in enumerate(messages):
            own[ks[at // PIECES], at % PIECES] = message

    def move(out, values, ks, piece):
        for k in ks:
            out[k, piece] = swap(values[k, piece], "seg", k) if k else values[k, piece]

    def arrived(ks):
        return [back[k, piece] for k in ks for piece in range(PIECES)]

    *parts, xs1, ys1, table = states_part(
        mid, late - mid, segs, place, x, dy, (delta, rates[None, :]), b, c
    )
    keep(mid_ks, parts)
    move(got, own, mid_ks, 0)
    *parts, xs2, ys2 = states_part(late, segs - late, segs, place, x, dy, (table,), b, c)
    keep(late_ks, parts)
    move(got, own, late_ks, 0)
    *parts, xs0, ys0 = states_part(0, mid, segs, place, x, dy, (table,), b, c)
    keep(near_ks, parts)
    move(got, own, near_ks, 0)
    for piece in range(1, PIECES):
        move(got, own, mid_ks, piece)
        move(got, own, late_ks, piece)
        move(got, own, near_ks, piece)
    low1, up1, gb1, gc1 = scores_part(mid, segs, width, place, (xs1, ys1, xs2, ys2), b, c)
    low0, up0, gb0, gc0 = scores_part(0, segs, width, place, (xs0, ys0), b, c)
    for piece in range(PIECES):
        sent = tree_chunk(segs, place, parents, [got[k, piece] for k in range(segs)])
        sent = {(k, piece): value for k, value in enumerate(sent)}
        move(back, sent, near_ks, piece)
        move(back, sent, mid_ks, piece)
        move(back, sent, late_ks, piece)
    skip = jnp.repeat(skips, P_SIZE)[None, :]
    grads0 = grads_part(0, segs, width, heads, place, arrived(near_ks), xs0, ys0, gb0, gc0)
    moved0 = [grads0[0]] + [swap(grads0[k], "head", k) for k in range(1, heads)]
    common = (table, low0, up0, skip, b, c)
    out, dx, sums = outputs_part(0, segs, place, arrived(near_ks), x, dy, xs0, ys0, *common)
    common = (table, low1, up1, skip, b, c)
    gb1, gc1 = grads_part(mid, segs, width, 0, place, arrived(mid_ks), xs1, ys1, gb1, gc1)
    out, dx, sums = outputs_part(
        mid, segs, place, arrived(mid_ks), x, dy, xs1, ys1, *common, (sums, out, dx)
    )
    out, dx, dd, *grads1 = outputs_part(
        late,
        segs,
        place,
        arrived(late_ks),
        x,
        dy,
        xs2,
        ys2,
        *common,
        (sums, out, dx),
        (delta, rates[:, None], gb1, gc1),
        heads,
    )
    moved1 = [grads1[0]] + [swap(grads1[k], "head", k) for k in range(1, heads)]
    gb, gc = place_grads(segs, place, moved0, moved1)
    return out[None], dx[None], dd[None], gb[None], gc[None]


def power_of_two(size):
    return size & (size - 1) == 0


def shards(inputs, deltas, rates, skips, writer, reader, grad_out, parents, levels):
    heads = deltas.shape[1]
    per_group_all = H // G
    local_groups = max(1, heads // per_group_all)
    members = max(1, per_group_all // heads)
    segs = lax.axis_size("seg")
    lanes = inputs.shape[2]
    even = power_of_two(segs) and power_of_two(lax.axis_size("head")) and segs >= 4
    if even and local_groups == 2 and heads == SLOTS and lanes // segs % TILE == 0:
        return paired(inputs, deltas, rates, skips, writer, reader, grad_out, parents)
    first_group = (lax.axis_index("head") * heads // per_group_all).astype(jnp.int32)[None]
    x, dy = inputs[0], grad_out[0]
    pad = SLOTS - heads
    delta = jnp.pad(deltas[0], ((0, pad), (0, 0)))
    rate = jnp.pad(rates, (0, pad))
    u, v, xs, ys, table, low, up, gb, gc = local_part(
        x, dy, delta, rate[None, :], writer[0], reader[0], first_group, local_groups
    )
    decay = jnp.repeat(jnp.exp(-rates * jnp.sum(deltas[0], axis=1)), P_SIZE)
    start, end = tree_states(u, v, decay, parents, levels)
    out, dx, gb, gc, dd = final_part(
        x,
        dy,
        xs,
        ys,
        start,
        end,
        u,
        table,
        low,
        up,
        gb,
        gc,
        jnp.repeat(skips, P_SIZE)[None, :],
        delta,
        rate[:, None],
        writer[0],
        reader[0],
        first_group,
        BF16 if members == 1 else F32,
    )
    grads = group_grads(gb, gc, members)
    return (out[None], dx[None], dd[None, :heads], grads[0][None], grads[1][None])


def solution(mesh):
    placed = (
        P("seg", None, "head"),
        P("seg", "head", None),
        P("head"),
        P("head"),
        P("seg", None, None),
        P("seg", None, None),
        P("seg", None, "head"),
        P(),
        P(),
    )
    return jax.shard_map(
        shards,
        mesh=mesh,
        in_specs=placed,
        out_specs=(
            P("seg", None, "head"),
            P("seg", None, "head"),
            P("seg", "head", None),
            P("seg", "head", None),
            P("seg", "head", None),
        ),
        check_vma=False,
    )
```

```python
import functools

import jax
import jax.numpy as jnp
from jax import lax
from jax.experimental import pallas as pl
from jax.experimental.pallas import tpu as pltpu
from jax.sharding import PartitionSpec as P


H = 256
P_SIZE = 64
N = 128
G = 8
DEPTH = 3
TILE = 256
SLOTS = 64
LANES = 128
EXTRA = 16
PIECES = 2

F32 = jnp.float32
BF16 = jnp.bfloat16


def dot(a, b, dims=((1,), (0,))):
    return lax.dot_general(a, b, (dims, ((), ())), preferred_element_type=F32)


NT = ((1,), (1,))


def split(value, parts):
    pieces = []
    for _ in range(parts):
        piece = value.astype(BF16)
        pieces.append(piece)
        value = value - piece.astype(F32)
    return pieces


def iota(shape, axis):
    return lax.broadcasted_iota(jnp.int32, shape, axis)


def onehot(cond):
    return jnp.where(cond, 1.0, 0.0).astype(BF16)


def spread(step):
    shape = (2 * SLOTS, TILE)
    head = step * (TILE // P_SIZE) + iota(shape, 1) // P_SIZE
    return onehot((iota(shape, 0) % SLOTS) == head)


def local_kernel(
    per_group,
    _,
    x_ref,
    dy_ref,
    delta_ref,
    rate_ref,
    b_ref,
    c_ref,
    u_ref,
    v_ref,
    xs_ref,
    ys_ref,
    table_ref,
    low_ref,
    up_ref,
    gb_ref,
    gc_ref,
    acc_ref,
):
    step = pl.program_id(0)
    length = x_ref.shape[0]
    square = (length, length)

    @pl.when(step == 0)
    def _():
        tri = onehot(iota(square, 0) >= iota(square, 1))
        eye = onehot(iota(square, 0) == iota(square, 1))
        pieces = split(delta_ref[...], 3)
        sums = sum(dot(tri, piece, NT) for piece in pieces)
        delta = sum(dot(eye, piece, NT) for piece in pieces)
        log = rate_ref[...] * sums
        grow = split(jnp.exp(log) * delta, 2)
        fall = split(jnp.exp(-log), 2)
        table_ref[0] = jnp.concatenate(fall, axis=1)
        table_ref[1] = jnp.concatenate(grow, axis=1)

    lanes = spread(step)
    fall = dot(table_ref[0], lanes)
    grow = dot(table_ref[1], lanes)
    xs, xs_low = split(x_ref[...].astype(F32) * grow, 2)
    ys, ys_low = split(dy_ref[...].astype(F32) * fall, 2)
    xs_ref[...] = xs
    ys_ref[...] = ys
    b, c = b_ref[...], c_ref[...]
    u = dot(b, xs, ((0,), (0,))) + dot(b, xs_low, ((0,), (0,)))
    v = dot(c, ys, ((0,), (0,))) + dot(c, ys_low, ((0,), (0,)))
    u_ref[...] = (u * fall[length - 1 :]).astype(BF16)
    v_ref[...] = v.astype(BF16)
    part = dot(ys, xs, NT)
    inner = step % per_group

    @pl.when(inner == 0)
    def _():
        acc_ref[...] = part

    @pl.when(inner > 0)
    def _():
        acc_ref[...] += part

    @pl.when(inner == per_group - 1)
    def _():
        lower = iota(square, 0) >= iota(square, 1)
        upper = iota(square, 0) <= iota(square, 1)
        low_ref[...] = jnp.where(lower, dot(c, b, NT), 0.0).astype(BF16)
        up_ref[...] = jnp.where(upper, dot(b, c, NT), 0.0).astype(BF16)
        high, low = split(jnp.where(lower, acc_ref[...], 0.0), 2)
        gc_ref[...] = dot(high, b) + dot(low, b)
        gb_ref[...] = dot(high, c, ((0,), (0,))) + dot(low, c, ((0,), (0,)))


def local_part(x, dy, delta, rate, writer, reader, first_group, local_groups):
    length, lanes = x.shape
    steps = lanes // TILE
    per_group = steps // local_groups
    tile = lambda rows: pl.BlockSpec((rows, TILE), lambda i, f: (0, i))
    whole = lambda *shape: pl.BlockSpec(shape, lambda i, f: (0,) * len(shape))
    group = lambda rows, cols: pl.BlockSpec((None, rows, cols), lambda i, f: (i // per_group, 0, 0))
    proj = pl.BlockSpec((length, N), lambda i, f: (0, f[0] + i // per_group))
    shape = jax.ShapeDtypeStruct
    return pl.pallas_call(
        functools.partial(local_kernel, per_group),
        grid_spec=pltpu.PrefetchScalarGridSpec(
            num_scalar_prefetch=1,
            grid=(steps,),
            in_specs=[
                tile(length),
                tile(length),
                whole(SLOTS, length),
                whole(1, SLOTS),
                proj,
                proj,
            ],
            out_specs=[
                tile(N),
                tile(N),
                tile(length),
                tile(length),
                whole(2, length, 2 * SLOTS),
                group(length, length),
                group(length, length),
                group(length, N),
                group(length, N),
            ],
            scratch_shapes=[pltpu.VMEM((length, length), F32)],
        ),
        out_shape=[
            shape((N, lanes), BF16),
            shape((N, lanes), BF16),
            shape((length, lanes), BF16),
            shape((length, lanes), BF16),
            shape((2, length, 2 * SLOTS), BF16),
            shape((local_groups, length, length), BF16),
            shape((local_groups, length, length), BF16),
            shape((local_groups, length, N), F32),
            shape((local_groups, length, N), F32),
        ],
        cost_estimate=pl.CostEstimate(
            flops=8 * length * lanes * length, transcendentals=0, bytes_accessed=12 * length * lanes
        ),
        name="local_part",
    )(first_group, x, dy, delta, rate, writer, reader)


def final_kernel(
    per_group,
    steps,
    _,
    x_ref,
    dy_ref,
    xs_ref,
    ys_ref,
    start_ref,
    end_ref,
    u_ref,
    table_ref,
    low_ref,
    up_ref,
    b_ref,
    c_ref,
    gb_in,
    gc_in,
    skip_ref,
    delta_ref,
    rate_ref,
    out_ref,
    dx_ref,
    gb_ref,
    gc_ref,
    dd_ref,
    sums_ref,
    accb_ref,
    accc_ref,
):
    step = pl.program_id(0)
    length = x_ref.shape[0]
    lanes = spread(step)
    fall = dot(table_ref[0], lanes)
    grow = dot(table_ref[1], lanes)
    xs, ys, start = xs_ref[...], ys_ref[...], start_ref[...]
    total = fall[length - 1 :]
    end = end_ref[...].astype(F32) * total
    end_high, end_low = split(end, 2)
    core = dot(low_ref[...], xs) + dot(c_ref[...], start)
    grad = dot(up_ref[...], ys) + dot(b_ref[...], end_high) + dot(b_ref[...], end_low)
    skip = skip_ref[...]
    out_ref[...] = (fall * core + skip * x_ref[...].astype(F32)).astype(out_ref.dtype)
    dx_ref[...] = (grow * grad + skip * dy_ref[...].astype(F32)).astype(dx_ref.dtype)

    inner = step % per_group

    @pl.when(inner == 0)
    def _():
        accb_ref[...] = gb_in[...]
        accc_ref[...] = gc_in[...]

    accc_ref[...] += dot(ys, start, NT)
    accb_ref[...] += dot(xs, end_high, NT) + dot(xs, end_low, NT)

    @pl.when(inner == per_group - 1)
    def _():
        gb_ref[...] = accb_ref[...].astype(gb_ref.dtype)
        gc_ref[...] = accc_ref[...].astype(gc_ref.dtype)

    direct = xs.astype(F32) * grad
    through = ys.astype(F32) * core - direct
    shape = (TILE, 2 * SLOTS)
    column = iota(shape, 1)
    head = step * (TILE // P_SIZE) + iota(shape, 0) // P_SIZE
    pick_through = onehot(column == head)
    pick_direct = onehot(column == head + SLOTS)
    high, low = split(through, 2)
    dhigh, dlow = split(direct, 2)
    rows = dot(high, pick_through) + dot(low, pick_through)
    rows = rows + dot(dhigh, pick_direct) + dot(dlow, pick_direct)

    @pl.when(step == 0)
    def _():
        sums_ref[...] = rows

    @pl.when(step > 0)
    def _():
        sums_ref[...] += rows

    held = u_ref[...].astype(F32) / total + start.astype(F32)
    last = jnp.sum(end * held, axis=0, keepdims=True)
    at_last = jnp.where(iota((8, TILE), 0) == 7, last, 0.0)
    high, low = split(at_last, 2)
    sums_ref[length - 8 :, :] += dot(high, pick_through) + dot(low, pick_through)

    @pl.when(step == steps - 1)
    def _():
        both = sums_ref[...].T
        square = (length, length)
        later = onehot(iota(square, 0) >= iota(square, 1))
        back = sum(dot(piece, later) for piece in split(both[:SLOTS], 3))
        dd_ref[...] = both[SLOTS:] / delta_ref[...] - rate_ref[...] * back


def final_part(
    x, dy, xs, ys, start, end, u, table, low, up, gb, gc, skip, delta, rate, writer, reader, first_group, grad_dtype
):
    length, lanes = x.shape
    steps = lanes // TILE
    local_groups = low.shape[0]
    per_group = steps // local_groups
    tile = lambda rows: pl.BlockSpec((rows, TILE), lambda i, f: (0, i))
    whole = lambda *shape: pl.BlockSpec(shape, lambda i, f: (0,) * len(shape))
    group = lambda rows, cols: pl.BlockSpec((None, rows, cols), lambda i, f: (i // per_group, 0, 0))
    proj = pl.BlockSpec((length, N), lambda i, f: (0, f[0] + i // per_group))
    shape = jax.ShapeDtypeStruct
    return pl.pallas_call(
        functools.partial(final_kernel, per_group, steps),
        grid_spec=pltpu.PrefetchScalarGridSpec(
            num_scalar_prefetch=1,
            grid=(steps,),
            in_specs=[
                tile(length),
                tile(length),
                tile(length),
                tile(length),
                tile(N),
                tile(N),
                tile(N),
                whole(2, length, 2 * SLOTS),
                group(length, length),
                group(length, length),
                proj,
                proj,
                group(length, N),
                group(length, N),
                tile(1),
                whole(SLOTS, length),
                whole(SLOTS, 1),
            ],
            out_specs=[
                tile(length),
                tile(length),
                pl.BlockSpec((length, N), lambda i, f: (0, i // per_group)),
                pl.BlockSpec((length, N), lambda i, f: (0, i // per_group)),
                whole(SLOTS, length),
            ],
            scratch_shapes=[
                pltpu.VMEM((length, 2 * SLOTS), F32),
                pltpu.VMEM((length, N), F32),
                pltpu.VMEM((length, N), F32),
            ],
        ),
        out_shape=[
            shape((length, lanes), BF16),
            shape((length, lanes), BF16),
            shape((length, local_groups * N), grad_dtype),
            shape((length, local_groups * N), grad_dtype),
            shape((SLOTS, length), F32),
        ],
        cost_estimate=pl.CostEstimate(
            flops=12 * length * lanes * length, transcendentals=0, bytes_accessed=16 * length * lanes
        ),
        name="final_part",
    )(
        first_group, x, dy, xs, ys, start, end, u, table, low, up, writer, reader, gb, gc, skip, delta, rate
    )


def tree_states(u, v, decay, parents, levels):
    segs = lax.axis_size("seg")
    lanes = u.shape[1]
    chunk = lanes // segs

    def spread_heads(state):
        parts = jnp.swapaxes(state.reshape(N, segs, chunk), 0, 1)
        return lax.all_to_all(parts, "seg", 0, 0)

    decay_all = lax.all_to_all(decay.reshape(segs, chunk), "seg", 0, 0)[:, None, :]
    u_all = spread_heads(u)
    v_all = spread_heads(v).astype(F32)
    safe = jnp.maximum(parents, 0)
    starts = jnp.zeros_like(u_all)
    for repeat in range(DEPTH - 1):
        ends = (decay_all * starts.astype(F32) + u_all.astype(F32)).astype(BF16)
        starts = jnp.where((levels == repeat + 1)[:, None, None], ends[safe], starts)
    link = (parents[None, :] == jnp.arange(segs)[:, None]).astype(F32)
    grad_end = jnp.zeros_like(v_all)
    for _ in range(DEPTH - 1):
        lifted = decay_all * grad_end + v_all
        grad_end = sum(link[:, c, None, None] * lifted[c][None] for c in range(segs))

    def gather_heads(state):
        parts = lax.all_to_all(state, "seg", 0, 0)
        return jnp.swapaxes(parts, 0, 1).reshape(N, lanes)

    return gather_heads(starts), gather_heads(grad_end.astype(BF16))


def group_grads(gb, gc, members):
    shards_ = lax.axis_size("head")
    both = jnp.stack([gb, gc])
    length, width = gb.shape
    parts = both.reshape(2, shards_, length // shards_, width)
    parts = lax.all_to_all(parts, "head", 1, 1)
    if members > 1:
        parts = parts.reshape(2, shards_ // members, members, length // shards_, width).sum(2)
    parts = jnp.swapaxes(parts, 1, 2).reshape(2, length // shards_, -1)
    return parts.astype(BF16)


def chunk_of(place, k):
    return jnp.bitwise_xor(place[1], k)


def group_of(chunk, segs):
    return chunk * 2 // segs


def message_rows(width):
    return 2 * N * (width // LANES // PIECES) + EXTRA


def pack_states(ref, block, top, bottom):
    row = 2 * N * block
    ref[row : row + N, :] = top
    ref[row + N : row + 2 * N, :] = bottom


def tail_rows(rows_of):
    rows = iota((EXTRA, LANES), 0)
    tail = jnp.zeros((EXTRA, LANES), F32)
    for block, row in rows_of:
        for piece, value in enumerate(split(row, 3)):
            tail = tail + jnp.where(rows == 3 * block + piece, value.astype(F32), 0.0)
    return tail


def tail_row(tail, block):
    rows = iota((EXTRA, LANES), 0)
    own = (rows >= 3 * block) & (rows < 3 * block + 3)
    return jnp.sum(jnp.where(own, tail.astype(F32), 0.0), axis=0, keepdims=True)


def tables(delta_ref, rate_ref):
    length = delta_ref.shape[1]
    square = (length, length)
    tri = onehot(iota(square, 0) >= iota(square, 1))
    eye = onehot(iota(square, 0) == iota(square, 1))
    pieces = split(delta_ref[...], 3)
    sums = sum(dot(tri, piece, NT) for piece in pieces)
    delta = sum(dot(eye, piece, NT) for piece in pieces)
    log = rate_ref[...] * sums
    grow = split(jnp.exp(log) * delta, 2)
    fall = split(jnp.exp(-log), 2)
    return jnp.concatenate(fall, axis=1), jnp.concatenate(grow, axis=1)


def spread_at(lane):
    shape = (2 * SLOTS, TILE)
    head = (lane + iota(shape, 1)) // P_SIZE
    return onehot((iota(shape, 0) % SLOTS) == head)


def states_kernel(first, lead, place, x_ref, dy_ref, *refs):
    if lead:
        delta_ref, rate_ref, b_ref, c_ref, *outs = refs
        *messages, xs_ref, ys_ref, table_ref, bt_ref, ct_ref = outs
    else:
        table_ref, b_ref, c_ref, *outs = refs
        *messages, xs_ref, ys_ref, bt_ref, ct_ref = outs
    step = pl.program_id(0)
    length, width = x_ref.shape

    @pl.when(step == 0)
    def _():
        if lead:
            table_ref[0], table_ref[1] = tables(delta_ref, rate_ref)
        bt_ref[...] = b_ref[...].T
        ct_ref[...] = c_ref[...].T

    chunk = chunk_of(place, step + first)
    made = []
    for at in range(0, width, TILE):
        cols = slice(at, at + TILE)
        lanes = spread_at(chunk * width + at)
        fall = dot(table_ref[0], lanes)
        grow = dot(table_ref[1], lanes)
        xs, xs_low = split(x_ref[:, cols].astype(F32) * grow, 2)
        ys, ys_low = split(dy_ref[:, cols].astype(F32) * fall, 2)
        xs_ref[:, cols] = xs
        ys_ref[:, cols] = ys
        total = fall[length - 1 :]
        u = (dot(bt_ref[...], xs) + dot(bt_ref[...], xs_low)) * total
        v = dot(ct_ref[...], ys) + dot(ct_ref[...], ys_low)
        for part in range(0, TILE, LANES):
            lane = slice(part, part + LANES)
            made.append((u[:, lane].astype(BF16), v[:, lane].astype(BF16), total[:, lane]))
    for at, message in enumerate(messages):

        @pl.when(step == at // PIECES)
        def _(message=message, piece=at % PIECES):
            blocks = len(made) // PIECES
            held = made[piece * blocks : (piece + 1) * blocks]
            for block, (u, v, _) in enumerate(held):
                pack_states(message, block, u, v)
            tail = tail_rows([(block, row) for block, (_, _, row) in enumerate(held)])
            message[message.shape[0] - EXTRA :, :] = tail.astype(BF16)


def part_specs(length, width, segs, first):
    tile = lambda rows: pl.BlockSpec((rows, width), lambda i, f: (0, chunk_of(f, first + i)))
    turn = lambda rows: pl.BlockSpec((rows, width), lambda i, f: (0, i))
    whole = lambda *shape: pl.BlockSpec(shape, lambda i, f: (0,) * len(shape))
    proj = pl.BlockSpec(
        (length, N), lambda i, f: (0, 2 * f[0] + group_of(chunk_of(f, first), segs))
    )
    return tile, turn, whole, proj


def states_part(first, count, segs, place, x, dy, given, writer, reader):
    length, lanes = x.shape
    width = lanes // segs
    lead = len(given) == 2
    tile, turn, whole, proj = part_specs(length, width, segs, first)
    shape = jax.ShapeDtypeStruct
    message = shape((message_rows(width), LANES), BF16)
    scaled = shape((length, count * width), BF16)
    table = shape((2, length, 2 * SLOTS), BF16)
    return pl.pallas_call(
        functools.partial(states_kernel, first, lead),
        grid_spec=pltpu.PrefetchScalarGridSpec(
            num_scalar_prefetch=1,
            grid=(count,),
            in_specs=[tile(length), tile(length)]
            + [whole(*value.shape) for value in given]
            + [proj, proj],
            out_specs=[whole(*message.shape)] * (count * PIECES)
            + [turn(length), turn(length)]
            + ([whole(*table.shape)] if lead else []),
            scratch_shapes=[pltpu.VMEM((N, length), BF16)] * 2,
        ),
        out_shape=[message] * (count * PIECES) + [scaled, scaled] + ([table] if lead else []),
        cost_estimate=pl.CostEstimate(
            flops=8 * length * count * width * length,
            transcendentals=0,
            bytes_accessed=16 * length * count * width,
        ),
    )(place, x, dy, *given, writer, reader)


def scores_kernel(count, pairs, _, __, *refs):
    scaled, (b_ref, c_ref) = refs[: 2 * pairs], refs[2 * pairs : 2 * pairs + 2]
    low_ref, up_ref, gb_ref, gc_ref, acc_ref = refs[2 * pairs + 2 :]
    step = pl.program_id(0)
    length = b_ref.shape[0]
    square = (length, length)
    part = sum(dot(scaled[2 * i + 1][...], scaled[2 * i][...], NT) for i in range(pairs))

    @pl.when(step == 0)
    def _():
        acc_ref[...] = part

    @pl.when(step > 0)
    def _():
        acc_ref[...] += part

    @pl.when(step == count - 1)
    def _():
        b, c = b_ref[...], c_ref[...]
        lower = iota(square, 0) >= iota(square, 1)
        upper = iota(square, 0) <= iota(square, 1)
        low_ref[...] = jnp.where(lower, dot(c, b, NT), 0.0).astype(BF16)
        up_ref[...] = jnp.where(upper, dot(b, c, NT), 0.0).astype(BF16)
        high, low = split(jnp.where(lower, acc_ref[...], 0.0), 2)
        gc_ref[...] = dot(high, b) + dot(low, b)
        gb_ref[...] = dot(high, c, ((0,), (0,))) + dot(low, c, ((0,), (0,)))


def scores_part(first, segs, width, place, scaled, writer, reader, after):
    length, lanes = scaled[0].shape
    count = lanes // width
    _, turn, whole, proj = part_specs(length, width, segs, first)
    shape = jax.ShapeDtypeStruct
    return pl.pallas_call(
        functools.partial(scores_kernel, count, len(scaled) // 2),
        grid_spec=pltpu.PrefetchScalarGridSpec(
            num_scalar_prefetch=1,
            grid=(count,),
            in_specs=[pl.BlockSpec(memory_space=pl.ANY)]
            + [turn(length)] * len(scaled)
            + [proj, proj],
            out_specs=[whole(length, length)] * 2 + [whole(length, N)] * 2,
            scratch_shapes=[pltpu.VMEM((length, length), F32)],
        ),
        out_shape=[shape((length, length), BF16)] * 2 + [shape((length, N), F32)] * 2,
        cost_estimate=pl.CostEstimate(
            flops=4 * length * lanes * length, transcendentals=0, bytes_accessed=8 * length * lanes
        ),
    )(place, after, *scaled, writer, reader)


def tree_kernel(segs, place, parents, *refs):
    got, tails = refs[:segs], refs[segs : 2 * segs]
    sent = refs[2 * segs : 3 * segs]
    all_ref, end_ref, decay_ref, tail_ref = refs[3 * segs :]
    block = pl.program_id(0)
    for k in range(segs):
        seg = chunk_of(place, k)
        all_ref[seg] = got[k][...]
        decay_ref[seg] = tail_row(tails[k][...], block)
    end_ref[...] = jnp.zeros_like(end_ref)

    for seg in range(segs):
        parent = parents[seg]
        near = jnp.maximum(parent, 0)
        above = jnp.where(parent >= 0, parents[near], -1)

        @pl.when(parent >= 0)
        def _():
            end_ref[near] += all_ref[seg, N:, :].astype(F32)

        @pl.when(above >= 0)
        def _():
            end_ref[jnp.maximum(above, 0)] += decay_ref[near] * all_ref[seg, N:, :].astype(F32)

    rows = iota((EXTRA, LANES), 0)
    for k in range(segs):
        seg = chunk_of(place, k)
        parent = parents[seg]
        near = jnp.maximum(parent, 0)
        above = jnp.where(parent >= 0, parents[near], -1)
        state = all_ref[near, :N, :].astype(F32)
        lifted = decay_ref[near] * all_ref[jnp.maximum(above, 0), :N, :].astype(F32)
        start = jnp.where(parent >= 0, state, 0.0) + jnp.where(above >= 0, lifted, 0.0)
        start = start.astype(BF16)
        own = decay_ref[seg]
        end = (own * end_ref[seg]).astype(BF16)
        held = start.astype(F32) + all_ref[seg, :N, :].astype(F32) / own
        last = jnp.sum(end.astype(F32) * held, axis=0, keepdims=True)
        at = pl.multiple_of(block * 2 * N, 2 * N)
        sent[k][pl.ds(at, N), :] = start
        sent[k][pl.ds(pl.multiple_of(at + N, N), N), :] = end
        tail = tail_rows([(block, last)])
        tail_ref[k] = jnp.where(block == 0, tail, tail_ref[k] + tail)

    @pl.when(block == pl.num_programs(0) - 1)
    def _():
        for k in range(segs):
            sent[k][sent[k].shape[0] - EXTRA :, :] = tail_ref[k].astype(BF16)


def tree_chunk(segs, place, parents, messages):
    rows, _ = messages[0].shape
    blocks = (rows - EXTRA) // (2 * N)
    state = pl.BlockSpec((2 * N, LANES), lambda i, f, p: (i, 0))
    tail = pl.BlockSpec((EXTRA, LANES), lambda i, f, p: (2 * N * blocks // EXTRA, 0))
    return pl.pallas_call(
        functools.partial(tree_kernel, segs),
        grid_spec=pltpu.PrefetchScalarGridSpec(
            num_scalar_prefetch=2,
            grid=(blocks,),
            in_specs=[state] * segs + [tail] * segs,
            out_specs=[pl.BlockSpec((rows, LANES), lambda i, f, p: (0, 0))] * segs,
            scratch_shapes=[
                pltpu.VMEM((segs, 2 * N, LANES), BF16),
                pltpu.VMEM((segs, N, LANES), F32),
                pltpu.VMEM((segs, 1, LANES), F32),
                pltpu.VMEM((segs, EXTRA, LANES), F32),
            ],
        ),
        out_shape=[jax.ShapeDtypeStruct((rows, LANES), BF16)] * segs,
        cost_estimate=pl.CostEstimate(flops=10**7, transcendentals=0, bytes_accessed=10**7),
        name="tree",
    )(place, parents, *messages, *messages)


def unpack(messages, state_ref, last_ref):
    blocks = state_ref.shape[1] // LANES // PIECES
    for piece, message in enumerate(messages):
        tail = message[2 * N * blocks :, :]
        for block in range(blocks):
            lane = (piece * blocks + block) * LANES
            cols = slice(lane, lane + LANES)
            state_ref[:, cols] = message[2 * N * block : 2 * N * (block + 1), :]
            if last_ref is not None:
                last_ref[:, cols] = tail_row(tail, block)


def grads_shapes(length, heads):
    if heads:
        return [jax.ShapeDtypeStruct((2, length // heads, N), BF16)] * heads
    return [jax.ShapeDtypeStruct((length, N), F32)] * 2


def give(place, outs, accb_ref, accc_ref):
    if outs[0].dtype == F32:
        outs[0][...] = accb_ref[...]
        outs[1][...] = accc_ref[...]
        return
    block = accb_ref.shape[0] // len(outs)
    for k, out in enumerate(outs):
        row = jnp.bitwise_xor(place[0], k) * block
        rows = pl.ds(pl.multiple_of(row, block), block)
        out[0] = accb_ref[rows, :].astype(BF16)
        out[1] = accc_ref[rows, :].astype(BF16)


def grads_kernel(count, place, *refs):
    messages, refs = refs[: count * PIECES], refs[count * PIECES :]
    xs_ref, ys_ref, gb_in, gc_in, *outs, accb_ref, accc_ref, state_ref = refs
    step = pl.program_id(0)

    @pl.when(step == 0)
    def _():
        accb_ref[...] = gb_in[...]
        accc_ref[...] = gc_in[...]

    for at in range(count):

        @pl.when(step == at)
        def _(parts=messages[at * PIECES : (at + 1) * PIECES]):
            unpack(parts, state_ref, None)

    accc_ref[...] += dot(ys_ref[...], state_ref[:N, :], NT)
    accb_ref[...] += dot(xs_ref[...], state_ref[N:, :], NT)

    @pl.when(step == count - 1)
    def _():
        give(place, outs, accb_ref, accc_ref)


def grads_part(first, segs, width, heads, place, messages, xs, ys, gb, gc):
    length, lanes = xs.shape
    count = lanes // width
    _, turn, whole, _ = part_specs(length, width, segs, first)
    outs = grads_shapes(length, heads)
    return pl.pallas_call(
        functools.partial(grads_kernel, count),
        grid_spec=pltpu.PrefetchScalarGridSpec(
            num_scalar_prefetch=1,
            grid=(count,),
            in_specs=[whole(*messages[0].shape)] * len(messages)
            + [turn(length)] * 2
            + [whole(length, N)] * 2,
            out_specs=[whole(*out.shape) for out in outs],
            scratch_shapes=[pltpu.VMEM((length, N), F32)] * 2 + [pltpu.VMEM((2 * N, width), BF16)],
        ),
        out_shape=outs,
        cost_estimate=pl.CostEstimate(
            flops=4 * length * count * width * N,
            transcendentals=0,
            bytes_accessed=8 * length * count * width,
        ),
    )(place, *messages, xs, ys, gb, gc)


def outputs_kernel(first, count, earlier, final, grads, place, *refs):
    messages, refs = refs[: count * PIECES], refs[count * PIECES :]
    x_ref, dy_ref, xs_ref, ys_ref, table_ref, low_ref, up_ref, b_ref, c_ref, skip_ref = refs[:10]
    refs = refs[10:]
    if earlier:
        sums_in, _, _, *refs = refs
    if final:
        delta_ref, rate_ref, *refs = refs
    if grads:
        gb_in, gc_in, *refs = refs
    out_ref, dx_ref, end_ref, *refs = refs
    *refs, state_ref, last_ref = refs
    sums_ref = refs.pop() if final else end_ref
    if grads:
        *outs, accb_ref, accc_ref = refs
    step = pl.program_id(0)
    length, width = x_ref.shape
    for at in range(count):

        @pl.when(step == at)
        def _(parts=messages[at * PIECES : (at + 1) * PIECES]):
            unpack(parts, state_ref, last_ref)

    @pl.when(step == 0)
    def _():
        if grads:
            accb_ref[...] = gb_in[...]
            accc_ref[...] = gc_in[...]
        sums_ref[...] = sums_in[...] if earlier else jnp.zeros_like(sums_ref)

    chunk = chunk_of(place, step + first)
    for at in range(0, width, TILE):
        cols = slice(at, at + TILE)
        lane = chunk * width + at
        lanes = spread_at(lane)
        fall = dot(table_ref[0], lanes)
        grow = dot(table_ref[1], lanes)
        xs, ys = xs_ref[:, cols], ys_ref[:, cols]
        start, end = state_ref[:N, cols], state_ref[N:, cols]
        core = dot(low_ref[...], xs) + dot(c_ref[...], start)
        grad = dot(up_ref[...], ys) + dot(b_ref[...], end)
        skip = skip_ref[:, cols]
        out_ref[:, cols] = (fall * core + skip * x_ref[:, cols].astype(F32)).astype(BF16)
        dx_ref[:, cols] = (grow * grad + skip * dy_ref[:, cols].astype(F32)).astype(BF16)
        if grads:
            accc_ref[...] += dot(ys, start, NT)
            accb_ref[...] += dot(xs, end, NT)
        direct = xs.astype(F32) * grad
        through = ys.astype(F32) * core - direct
        shape = (TILE, 2 * SLOTS)
        column = iota(shape, 1)
        head = (lane + iota(shape, 0)) // P_SIZE
        pick_through = onehot(column == head)
        pick_direct = onehot(column == head + SLOTS)
        high, low = split(through, 2)
        dhigh, dlow = split(direct, 2)
        rows = dot(high, pick_through) + dot(low, pick_through)
        sums_ref[...] += rows + dot(dhigh, pick_direct) + dot(dlow, pick_direct)
        at_last = jnp.where(iota((8, TILE), 0) == 7, last_ref[:, cols], 0.0)
        high, low = split(at_last, 2)
        sums_ref[length - 8 :, :] += dot(high, pick_through) + dot(low, pick_through)

    if grads:

        @pl.when(step == count - 1)
        def _():
            give(place, outs, accb_ref, accc_ref)

    if final:

        @pl.when(step == count - 1)
        def _():
            rate = jnp.concatenate([rate_ref[...], jnp.ones_like(rate_ref)], axis=1)
            both = (sums_ref[...] * rate).T
            square = (length, length)
            later = onehot(iota(square, 0) >= iota(square, 1))
            back = sum(dot(piece, later) for piece in split(both[:SLOTS], 3))
            end_ref[...] = both[SLOTS:] / delta_ref[...] - back


def outputs_part(first, segs, place, messages, x, dy, xs, ys, table, low, up, skip, writer, reader, earlier=(), final=(), grads=(), heads=0):
    length, lanes = x.shape
    width = lanes // segs
    count = len(messages) // PIECES
    tile, turn, whole, proj = part_specs(length, width, segs, first)
    shape = jax.ShapeDtypeStruct
    sums = shape((length, 2 * SLOTS), F32)
    full = shape((length, lanes), BF16)
    any_ = pl.BlockSpec(memory_space=pl.ANY)
    in_specs = (
        [whole(*messages[0].shape)] * len(messages)
        + [tile(length), tile(length), turn(length), turn(length)]
        + [whole(*table.shape), whole(length, length), whole(length, length), proj, proj]
        + [tile(1)]
    )
    args = [*messages, x, dy, xs, ys, table, low, up, writer, reader, skip]
    aliases = {}
    if earlier:
        in_specs += [whole(*sums.shape), any_, any_]
        args += list(earlier)
        aliases = {len(args) - 1: 0, len(args): 1}
    in_specs += [whole(*value.shape) for value in (*final, *grads)]
    args += [*final, *grads]
    scratch = [pltpu.VMEM((2 * N, width), BF16), pltpu.VMEM((1, width), F32)]
    out_specs, out_shape = [tile(length), tile(length)], [full, full]
    end = shape(final[0].shape, F32) if final else sums
    out_specs.append(whole(*end.shape))
    out_shape.append(end)
    if final:
        scratch = [pltpu.VMEM(sums.shape, F32)] + scratch
    if grads:
        scratch = [pltpu.VMEM((length, N), F32)] * 2 + scratch
        given = grads_shapes(length, heads)
        out_specs += [whole(*value.shape) for value in given]
        out_shape += given
    return pl.pallas_call(
        functools.partial(
            outputs_kernel, first, count, bool(earlier), bool(final), bool(grads)
        ),
        grid_spec=pltpu.PrefetchScalarGridSpec(
            num_scalar_prefetch=1,
            grid=(count,),
            in_specs=in_specs,
            out_specs=out_specs,
            scratch_shapes=scratch,
        ),
        out_shape=out_shape,
        input_output_aliases=aliases,
        cost_estimate=pl.CostEstimate(
            flops=12 * length * count * width * length,
            transcendentals=0,
            bytes_accessed=16 * length * count * width,
        ),
    )(place, *args)


def place_kernel(heads, segs, place, *refs):
    near, far, (gb_ref, gc_ref) = refs[:heads], refs[heads : 2 * heads], refs[2 * heads :]
    for k in range(heads):
        owner = jnp.bitwise_xor(place[0], k)
        for half, parts in enumerate((near, far)):
            group = 2 * owner + group_of(chunk_of(place, half * segs // 2), segs)
            cols = pl.ds(pl.multiple_of(group * N, N), N)
            gb_ref[:, cols] = parts[k][0]
            gc_ref[:, cols] = parts[k][1]


def place_grads(segs, place, near, far):
    heads = len(near)
    rows = near[0].shape[1]
    shape = jax.ShapeDtypeStruct((rows, 2 * heads * N), BF16)
    return pl.pallas_call(
        functools.partial(place_kernel, heads, segs),
        grid_spec=pltpu.PrefetchScalarGridSpec(
            num_scalar_prefetch=1,
            grid=(1,),
            in_specs=[pl.BlockSpec(near[0].shape, lambda i, f: (0, 0, 0))] * (2 * heads),
            out_specs=[pl.BlockSpec(shape.shape, lambda i, f: (0, 0))] * 2,
        ),
        out_shape=[shape] * 2,
        name="place_grads",
    )(place, *near, *far)


def swap(value, axis, k):
    size = lax.axis_size(axis)
    return lax.ppermute(value, axis, [(i, i ^ k) for i in range(size)])


def paired(inputs, deltas, rates, skips, writer, reader, grad_out, parents):
    segs = lax.axis_size("seg")
    heads = lax.axis_size("head")
    mid, late = segs // 2, 3 * segs // 4
    near_ks, mid_ks, late_ks = range(mid), range(mid, late), range(late, segs)
    place = jnp.stack([lax.axis_index("head"), lax.axis_index("seg")]).astype(jnp.int32)
    x, dy, b, c = inputs[0], grad_out[0], writer[0], reader[0]
    width = x.shape[1] // segs
    delta = deltas[0]
    own, got, back = {}, {}, {}

    def keep(ks, messages):
        for at, message in enumerate(messages):
            own[ks[at // PIECES], at % PIECES] = message

    def move(out, values, ks, piece):
        for k in ks:
            out[k, piece] = swap(values[k, piece], "seg", k) if k else values[k, piece]

    def arrived(ks):
        return [back[k, piece] for k in ks for piece in range(PIECES)]

    *parts, xs1, ys1, table = states_part(
        mid, late - mid, segs, place, x, dy, (delta, rates[None, :]), b, c
    )
    keep(mid_ks, parts)
    move(got, own, mid_ks, 0)
    *parts, xs2, ys2 = states_part(late, segs - late, segs, place, x, dy, (table,), b, c)
    keep(late_ks, parts)
    move(got, own, late_ks, 0)
    *parts, xs0, ys0 = states_part(0, mid, segs, place, x, dy, (table,), b, c)
    keep(near_ks, parts)
    move(got, own, near_ks, 0)
    for piece in range(1, PIECES):
        move(got, own, mid_ks, piece)
        move(got, own, late_ks, piece)
        move(got, own, near_ks, piece)
    skip = jnp.repeat(skips, P_SIZE)[None, :]
    scaled = (xs1, ys1, xs2, ys2)
    low1, up1, gb1, gc1 = scores_part(mid, segs, width, place, scaled, b, c, skip)
    low0, up0, gb0, gc0 = scores_part(0, segs, width, place, (xs0, ys0), b, c, skip)
    for piece in range(PIECES):
        sent = tree_chunk(segs, place, parents, [got[k, piece] for k in range(segs)])
        sent = {(k, piece): value for k, value in enumerate(sent)}
        move(back, sent, near_ks, piece)
        move(back, sent, mid_ks, piece)
        move(back, sent, late_ks, piece)
    common = (table, low0, up0, skip, b, c)
    out, dx, sums, *grads0 = outputs_part(
        0,
        segs,
        place,
        arrived(near_ks),
        x,
        dy,
        xs0,
        ys0,
        *common,
        grads=(gb0, gc0),
        heads=heads,
    )
    moved0 = [grads0[0]] + [swap(grads0[k], "head", k) for k in range(1, heads)]
    common = (table, low1, up1, skip, b, c)
    out, dx, sums, gb1, gc1 = outputs_part(
        mid,
        segs,
        place,
        arrived(mid_ks),
        x,
        dy,
        xs1,
        ys1,
        *common,
        earlier=(sums, out, dx),
        grads=(gb1, gc1),
    )
    grads1 = grads_part(late, segs, width, heads, place, arrived(late_ks), xs2, ys2, gb1, gc1)
    moved1 = [grads1[0]] + [swap(grads1[k], "head", k) for k in range(1, heads)]
    out, dx, dd = outputs_part(
        late,
        segs,
        place,
        arrived(late_ks),
        x,
        dy,
        xs2,
        ys2,
        *common,
        earlier=(sums, out, dx),
        final=(delta, rates[None, :]),
    )
    gb, gc = place_grads(segs, place, moved0, moved1)
    return out[None], dx[None], dd[None], gb[None], gc[None]


def power_of_two(size):
    return size & (size - 1) == 0


def shards(inputs, deltas, rates, skips, writer, reader, grad_out, parents, levels):
    heads = deltas.shape[1]
    per_group_all = H // G
    local_groups = max(1, heads // per_group_all)
    members = max(1, per_group_all // heads)
    segs = lax.axis_size("seg")
    lanes = inputs.shape[2]
    even = power_of_two(segs) and power_of_two(lax.axis_size("head")) and segs >= 4
    if even and local_groups == 2 and heads == SLOTS and lanes // segs % TILE == 0:
        return paired(inputs, deltas, rates, skips, writer, reader, grad_out, parents)
    first_group = (lax.axis_index("head") * heads // per_group_all).astype(jnp.int32)[None]
    x, dy = inputs[0], grad_out[0]
    pad = SLOTS - heads
    delta = jnp.pad(deltas[0], ((0, pad), (0, 0)))
    rate = jnp.pad(rates, (0, pad))
    u, v, xs, ys, table, low, up, gb, gc = local_part(
        x, dy, delta, rate[None, :], writer[0], reader[0], first_group, local_groups
    )
    decay = jnp.repeat(jnp.exp(-rates * jnp.sum(deltas[0], axis=1)), P_SIZE)
    start, end = tree_states(u, v, decay, parents, levels)
    out, dx, gb, gc, dd = final_part(
        x,
        dy,
        xs,
        ys,
        start,
        end,
        u,
        table,
        low,
        up,
        gb,
        gc,
        jnp.repeat(skips, P_SIZE)[None, :],
        delta,
        rate[:, None],
        writer[0],
        reader[0],
        first_group,
        BF16 if members == 1 else F32,
    )
    grads = group_grads(gb, gc, members)
    return (out[None], dx[None], dd[None, :heads], grads[0][None], grads[1][None])


def solution(mesh):
    placed = (
        P("seg", None, "head"),
        P("seg", "head", None),
        P("head"),
        P("head"),
        P("seg", None, None),
        P("seg", None, None),
        P("seg", None, "head"),
        P(),
        P(),
    )
    return jax.shard_map(
        shards,
        mesh=mesh,
        in_specs=placed,
        out_specs=(
            P("seg", None, "head"),
            P("seg", None, "head"),
            P("seg", "head", None),
            P("seg", "head", None),
            P("seg", "head", None),
        ),
        check_vma=False,
    )
```

```python
import functools

import jax
import jax.numpy as jnp
from jax import lax
from jax.experimental import pallas as pl
from jax.experimental.pallas import tpu as pltpu
from jax.sharding import PartitionSpec as P


H = 256
P_SIZE = 64
N = 128
G = 8
DEPTH = 3
TILE = 256
SLOTS = 64
LANES = 128
EXTRA = 16
PIECES = 2

F32 = jnp.float32
BF16 = jnp.bfloat16


def dot(a, b, dims=((1,), (0,))):
    return lax.dot_general(a, b, (dims, ((), ())), preferred_element_type=F32)


NT = ((1,), (1,))


def split(value, parts):
    pieces = []
    for _ in range(parts):
        piece = value.astype(BF16)
        pieces.append(piece)
        value = value - piece.astype(F32)
    return pieces


def iota(shape, axis):
    return lax.broadcasted_iota(jnp.int32, shape, axis)


def onehot(cond):
    return jnp.where(cond, 1.0, 0.0).astype(BF16)


def spread(step):
    shape = (2 * SLOTS, TILE)
    head = step * (TILE // P_SIZE) + iota(shape, 1) // P_SIZE
    return onehot((iota(shape, 0) % SLOTS) == head)


def local_kernel(
    per_group,
    _,
    x_ref,
    dy_ref,
    delta_ref,
    rate_ref,
    b_ref,
    c_ref,
    u_ref,
    v_ref,
    xs_ref,
    ys_ref,
    table_ref,
    low_ref,
    up_ref,
    gb_ref,
    gc_ref,
    acc_ref,
):
    step = pl.program_id(0)
    length = x_ref.shape[0]
    square = (length, length)

    @pl.when(step == 0)
    def _():
        tri = onehot(iota(square, 0) >= iota(square, 1))
        eye = onehot(iota(square, 0) == iota(square, 1))
        pieces = split(delta_ref[...], 3)
        sums = sum(dot(tri, piece, NT) for piece in pieces)
        delta = sum(dot(eye, piece, NT) for piece in pieces)
        log = rate_ref[...] * sums
        grow = split(jnp.exp(log) * delta, 2)
        fall = split(jnp.exp(-log), 2)
        table_ref[0] = jnp.concatenate(fall, axis=1)
        table_ref[1] = jnp.concatenate(grow, axis=1)

    lanes = spread(step)
    fall = dot(table_ref[0], lanes)
    grow = dot(table_ref[1], lanes)
    xs, xs_low = split(x_ref[...].astype(F32) * grow, 2)
    ys, ys_low = split(dy_ref[...].astype(F32) * fall, 2)
    xs_ref[...] = xs
    ys_ref[...] = ys
    b, c = b_ref[...], c_ref[...]
    u = dot(b, xs, ((0,), (0,))) + dot(b, xs_low, ((0,), (0,)))
    v = dot(c, ys, ((0,), (0,))) + dot(c, ys_low, ((0,), (0,)))
    u_ref[...] = (u * fall[length - 1 :]).astype(BF16)
    v_ref[...] = v.astype(BF16)
    part = dot(ys, xs, NT)
    inner = step % per_group

    @pl.when(inner == 0)
    def _():
        acc_ref[...] = part

    @pl.when(inner > 0)
    def _():
        acc_ref[...] += part

    @pl.when(inner == per_group - 1)
    def _():
        lower = iota(square, 0) >= iota(square, 1)
        upper = iota(square, 0) <= iota(square, 1)
        low_ref[...] = jnp.where(lower, dot(c, b, NT), 0.0).astype(BF16)
        up_ref[...] = jnp.where(upper, dot(b, c, NT), 0.0).astype(BF16)
        high, low = split(jnp.where(lower, acc_ref[...], 0.0), 2)
        gc_ref[...] = dot(high, b) + dot(low, b)
        gb_ref[...] = dot(high, c, ((0,), (0,))) + dot(low, c, ((0,), (0,)))


def local_part(x, dy, delta, rate, writer, reader, first_group, local_groups):
    length, lanes = x.shape
    steps = lanes // TILE
    per_group = steps // local_groups
    tile = lambda rows: pl.BlockSpec((rows, TILE), lambda i, f: (0, i))
    whole = lambda *shape: pl.BlockSpec(shape, lambda i, f: (0,) * len(shape))
    group = lambda rows, cols: pl.BlockSpec((None, rows, cols), lambda i, f: (i // per_group, 0, 0))
    proj = pl.BlockSpec((length, N), lambda i, f: (0, f[0] + i // per_group))
    shape = jax.ShapeDtypeStruct
    return pl.pallas_call(
        functools.partial(local_kernel, per_group),
        grid_spec=pltpu.PrefetchScalarGridSpec(
            num_scalar_prefetch=1,
            grid=(steps,),
            in_specs=[
                tile(length),
                tile(length),
                whole(SLOTS, length),
                whole(1, SLOTS),
                proj,
                proj,
            ],
            out_specs=[
                tile(N),
                tile(N),
                tile(length),
                tile(length),
                whole(2, length, 2 * SLOTS),
                group(length, length),
                group(length, length),
                group(length, N),
                group(length, N),
            ],
            scratch_shapes=[pltpu.VMEM((length, length), F32)],
        ),
        out_shape=[
            shape((N, lanes), BF16),
            shape((N, lanes), BF16),
            shape((length, lanes), BF16),
            shape((length, lanes), BF16),
            shape((2, length, 2 * SLOTS), BF16),
            shape((local_groups, length, length), BF16),
            shape((local_groups, length, length), BF16),
            shape((local_groups, length, N), F32),
            shape((local_groups, length, N), F32),
        ],
        cost_estimate=pl.CostEstimate(
            flops=8 * length * lanes * length, transcendentals=0, bytes_accessed=12 * length * lanes
        ),
        name="local_part",
    )(first_group, x, dy, delta, rate, writer, reader)


def final_kernel(
    per_group,
    steps,
    _,
    x_ref,
    dy_ref,
    xs_ref,
    ys_ref,
    start_ref,
    end_ref,
    u_ref,
    table_ref,
    low_ref,
    up_ref,
    b_ref,
    c_ref,
    gb_in,
    gc_in,
    skip_ref,
    delta_ref,
    rate_ref,
    out_ref,
    dx_ref,
    gb_ref,
    gc_ref,
    dd_ref,
    sums_ref,
    accb_ref,
    accc_ref,
):
    step = pl.program_id(0)
    length = x_ref.shape[0]
    lanes = spread(step)
    fall = dot(table_ref[0], lanes)
    grow = dot(table_ref[1], lanes)
    xs, ys, start = xs_ref[...], ys_ref[...], start_ref[...]
    total = fall[length - 1 :]
    end = end_ref[...].astype(F32) * total
    end_high, end_low = split(end, 2)
    core = dot(low_ref[...], xs) + dot(c_ref[...], start)
    grad = dot(up_ref[...], ys) + dot(b_ref[...], end_high) + dot(b_ref[...], end_low)
    skip = skip_ref[...]
    out_ref[...] = (fall * core + skip * x_ref[...].astype(F32)).astype(out_ref.dtype)
    dx_ref[...] = (grow * grad + skip * dy_ref[...].astype(F32)).astype(dx_ref.dtype)

    inner = step % per_group

    @pl.when(inner == 0)
    def _():
        accb_ref[...] = gb_in[...]
        accc_ref[...] = gc_in[...]

    accc_ref[...] += dot(ys, start, NT)
    accb_ref[...] += dot(xs, end_high, NT) + dot(xs, end_low, NT)

    @pl.when(inner == per_group - 1)
    def _():
        gb_ref[...] = accb_ref[...].astype(gb_ref.dtype)
        gc_ref[...] = accc_ref[...].astype(gc_ref.dtype)

    direct = xs.astype(F32) * grad
    through = ys.astype(F32) * core - direct
    shape = (TILE, 2 * SLOTS)
    column = iota(shape, 1)
    head = step * (TILE // P_SIZE) + iota(shape, 0) // P_SIZE
    pick_through = onehot(column == head)
    pick_direct = onehot(column == head + SLOTS)
    high, low = split(through, 2)
    dhigh, dlow = split(direct, 2)
    rows = dot(high, pick_through) + dot(low, pick_through)
    rows = rows + dot(dhigh, pick_direct) + dot(dlow, pick_direct)

    @pl.when(step == 0)
    def _():
        sums_ref[...] = rows

    @pl.when(step > 0)
    def _():
        sums_ref[...] += rows

    held = u_ref[...].astype(F32) / total + start.astype(F32)
    last = jnp.sum(end * held, axis=0, keepdims=True)
    at_last = jnp.where(iota((8, TILE), 0) == 7, last, 0.0)
    high, low = split(at_last, 2)
    sums_ref[length - 8 :, :] += dot(high, pick_through) + dot(low, pick_through)

    @pl.when(step == steps - 1)
    def _():
        both = sums_ref[...].T
        square = (length, length)
        later = onehot(iota(square, 0) >= iota(square, 1))
        back = sum(dot(piece, later) for piece in split(both[:SLOTS], 3))
        dd_ref[...] = both[SLOTS:] / delta_ref[...] - rate_ref[...] * back


def final_part(
    x, dy, xs, ys, start, end, u, table, low, up, gb, gc, skip, delta, rate, writer, reader, first_group, grad_dtype
):
    length, lanes = x.shape
    steps = lanes // TILE
    local_groups = low.shape[0]
    per_group = steps // local_groups
    tile = lambda rows: pl.BlockSpec((rows, TILE), lambda i, f: (0, i))
    whole = lambda *shape: pl.BlockSpec(shape, lambda i, f: (0,) * len(shape))
    group = lambda rows, cols: pl.BlockSpec((None, rows, cols), lambda i, f: (i // per_group, 0, 0))
    proj = pl.BlockSpec((length, N), lambda i, f: (0, f[0] + i // per_group))
    shape = jax.ShapeDtypeStruct
    return pl.pallas_call(
        functools.partial(final_kernel, per_group, steps),
        grid_spec=pltpu.PrefetchScalarGridSpec(
            num_scalar_prefetch=1,
            grid=(steps,),
            in_specs=[
                tile(length),
                tile(length),
                tile(length),
                tile(length),
                tile(N),
                tile(N),
                tile(N),
                whole(2, length, 2 * SLOTS),
                group(length, length),
                group(length, length),
                proj,
                proj,
                group(length, N),
                group(length, N),
                tile(1),
                whole(SLOTS, length),
                whole(SLOTS, 1),
            ],
            out_specs=[
                tile(length),
                tile(length),
                pl.BlockSpec((length, N), lambda i, f: (0, i // per_group)),
                pl.BlockSpec((length, N), lambda i, f: (0, i // per_group)),
                whole(SLOTS, length),
            ],
            scratch_shapes=[
                pltpu.VMEM((length, 2 * SLOTS), F32),
                pltpu.VMEM((length, N), F32),
                pltpu.VMEM((length, N), F32),
            ],
        ),
        out_shape=[
            shape((length, lanes), BF16),
            shape((length, lanes), BF16),
            shape((length, local_groups * N), grad_dtype),
            shape((length, local_groups * N), grad_dtype),
            shape((SLOTS, length), F32),
        ],
        cost_estimate=pl.CostEstimate(
            flops=12 * length * lanes * length, transcendentals=0, bytes_accessed=16 * length * lanes
        ),
        name="final_part",
    )(
        first_group, x, dy, xs, ys, start, end, u, table, low, up, writer, reader, gb, gc, skip, delta, rate
    )


def tree_states(u, v, decay, parents, levels):
    segs = lax.axis_size("seg")
    lanes = u.shape[1]
    chunk = lanes // segs

    def spread_heads(state):
        parts = jnp.swapaxes(state.reshape(N, segs, chunk), 0, 1)
        return lax.all_to_all(parts, "seg", 0, 0)

    decay_all = lax.all_to_all(decay.reshape(segs, chunk), "seg", 0, 0)[:, None, :]
    u_all = spread_heads(u)
    v_all = spread_heads(v).astype(F32)
    safe = jnp.maximum(parents, 0)
    starts = jnp.zeros_like(u_all)
    for repeat in range(DEPTH - 1):
        ends = (decay_all * starts.astype(F32) + u_all.astype(F32)).astype(BF16)
        starts = jnp.where((levels == repeat + 1)[:, None, None], ends[safe], starts)
    link = (parents[None, :] == jnp.arange(segs)[:, None]).astype(F32)
    grad_end = jnp.zeros_like(v_all)
    for _ in range(DEPTH - 1):
        lifted = decay_all * grad_end + v_all
        grad_end = sum(link[:, c, None, None] * lifted[c][None] for c in range(segs))

    def gather_heads(state):
        parts = lax.all_to_all(state, "seg", 0, 0)
        return jnp.swapaxes(parts, 0, 1).reshape(N, lanes)

    return gather_heads(starts), gather_heads(grad_end.astype(BF16))


def group_grads(gb, gc, members):
    shards_ = lax.axis_size("head")
    both = jnp.stack([gb, gc])
    length, width = gb.shape
    parts = both.reshape(2, shards_, length // shards_, width)
    parts = lax.all_to_all(parts, "head", 1, 1)
    if members > 1:
        parts = parts.reshape(2, shards_ // members, members, length // shards_, width).sum(2)
    parts = jnp.swapaxes(parts, 1, 2).reshape(2, length // shards_, -1)
    return parts.astype(BF16)


def chunk_of(place, k):
    return jnp.bitwise_xor(place[1], k)


def group_of(chunk, segs):
    return chunk * 2 // segs


def message_rows(width):
    return 2 * N * (width // LANES // PIECES) + EXTRA


def pack_states(ref, block, top, bottom):
    row = 2 * N * block
    ref[row : row + N, :] = top
    ref[row + N : row + 2 * N, :] = bottom


def tail_rows(rows_of):
    rows = iota((EXTRA, LANES), 0)
    tail = jnp.zeros((EXTRA, LANES), F32)
    for block, row in rows_of:
        for piece, value in enumerate(split(row, 3)):
            tail = tail + jnp.where(rows == 3 * block + piece, value.astype(F32), 0.0)
    return tail


def tail_row(tail, block):
    rows = iota((EXTRA, LANES), 0)
    own = (rows >= 3 * block) & (rows < 3 * block + 3)
    return jnp.sum(jnp.where(own, tail.astype(F32), 0.0), axis=0, keepdims=True)


def tables(delta_ref, rate_ref):
    length = delta_ref.shape[1]
    square = (length, length)
    tri = onehot(iota(square, 0) >= iota(square, 1))
    eye = onehot(iota(square, 0) == iota(square, 1))
    pieces = split(delta_ref[...], 3)
    sums = sum(dot(tri, piece, NT) for piece in pieces)
    delta = sum(dot(eye, piece, NT) for piece in pieces)
    log = rate_ref[...] * sums
    grow = split(jnp.exp(log) * delta, 2)
    fall = split(jnp.exp(-log), 2)
    return jnp.concatenate(fall, axis=1), jnp.concatenate(grow, axis=1)


def spread_at(lane):
    shape = (2 * SLOTS, TILE)
    head = (lane + iota(shape, 1)) // P_SIZE
    return onehot((iota(shape, 0) % SLOTS) == head)


def states_kernel(first, lead, place, x_ref, dy_ref, *refs):
    if lead:
        delta_ref, rate_ref, b_ref, c_ref, *outs = refs
        *messages, xs_ref, ys_ref, table_ref, bt_ref, ct_ref = outs
    else:
        table_ref, b_ref, c_ref, *outs = refs
        *messages, xs_ref, ys_ref, bt_ref, ct_ref = outs
    step = pl.program_id(0)
    length, width = x_ref.shape

    @pl.when(step == 0)
    def _():
        if lead:
            table_ref[0], table_ref[1] = tables(delta_ref, rate_ref)
        bt_ref[...] = b_ref[...].T
        ct_ref[...] = c_ref[...].T

    chunk = chunk_of(place, step + first)
    made = []
    for at in range(0, width, TILE):
        cols = slice(at, at + TILE)
        lanes = spread_at(chunk * width + at)
        fall = dot(table_ref[0], lanes)
        grow = dot(table_ref[1], lanes)
        xs, xs_low = split(x_ref[:, cols].astype(F32) * grow, 2)
        ys, ys_low = split(dy_ref[:, cols].astype(F32) * fall, 2)
        xs_ref[:, cols] = xs
        ys_ref[:, cols] = ys
        total = fall[length - 1 :]
        u = (dot(bt_ref[...], xs) + dot(bt_ref[...], xs_low)) * total
        v = dot(ct_ref[...], ys) + dot(ct_ref[...], ys_low)
        for part in range(0, TILE, LANES):
            lane = slice(part, part + LANES)
            made.append((u[:, lane].astype(BF16), v[:, lane].astype(BF16), total[:, lane]))
    for at, message in enumerate(messages):

        @pl.when(step == at // PIECES)
        def _(message=message, piece=at % PIECES):
            blocks = len(made) // PIECES
            held = made[piece * blocks : (piece + 1) * blocks]
            for block, (u, v, _) in enumerate(held):
                pack_states(message, block, u, v)
            tail = tail_rows([(block, row) for block, (_, _, row) in enumerate(held)])
            message[message.shape[0] - EXTRA :, :] = tail.astype(BF16)


def part_specs(length, width, segs, first, pieces=1, piece=0):
    part = width // pieces
    tile = lambda rows: pl.BlockSpec(
        (rows, part), lambda i, f: (0, chunk_of(f, first + i) * pieces + piece)
    )
    turn = lambda rows: pl.BlockSpec((rows, part), lambda i, f: (0, i * pieces + piece))
    whole = lambda *shape: pl.BlockSpec(shape, lambda i, f: (0,) * len(shape))
    proj = pl.BlockSpec(
        (length, N), lambda i, f: (0, 2 * f[0] + group_of(chunk_of(f, first), segs))
    )
    return tile, turn, whole, proj


def states_part(first, count, segs, place, x, dy, given, writer, reader):
    length, lanes = x.shape
    width = lanes // segs
    lead = len(given) == 2
    tile, turn, whole, proj = part_specs(length, width, segs, first)
    shape = jax.ShapeDtypeStruct
    message = shape((message_rows(width), LANES), BF16)
    scaled = shape((length, count * width), BF16)
    table = shape((2, length, 2 * SLOTS), BF16)
    return pl.pallas_call(
        functools.partial(states_kernel, first, lead),
        grid_spec=pltpu.PrefetchScalarGridSpec(
            num_scalar_prefetch=1,
            grid=(count,),
            in_specs=[tile(length), tile(length)]
            + [whole(*value.shape) for value in given]
            + [proj, proj],
            out_specs=[whole(*message.shape)] * (count * PIECES)
            + [turn(length), turn(length)]
            + ([whole(*table.shape)] if lead else []),
            scratch_shapes=[pltpu.VMEM((N, length), BF16)] * 2,
        ),
        out_shape=[message] * (count * PIECES) + [scaled, scaled] + ([table] if lead else []),
        cost_estimate=pl.CostEstimate(
            flops=8 * length * count * width * length,
            transcendentals=0,
            bytes_accessed=16 * length * count * width,
        ),
    )(place, x, dy, *given, writer, reader)


def scores_kernel(count, pairs, _, __, *refs):
    scaled, (b_ref, c_ref) = refs[: 2 * pairs], refs[2 * pairs : 2 * pairs + 2]
    low_ref, up_ref, gb_ref, gc_ref, acc_ref = refs[2 * pairs + 2 :]
    step = pl.program_id(0)
    length = b_ref.shape[0]
    square = (length, length)
    part = sum(dot(scaled[2 * i + 1][...], scaled[2 * i][...], NT) for i in range(pairs))

    @pl.when(step == 0)
    def _():
        acc_ref[...] = part

    @pl.when(step > 0)
    def _():
        acc_ref[...] += part

    @pl.when(step == count - 1)
    def _():
        b, c = b_ref[...], c_ref[...]
        lower = iota(square, 0) >= iota(square, 1)
        upper = iota(square, 0) <= iota(square, 1)
        low_ref[...] = jnp.where(lower, dot(c, b, NT), 0.0).astype(BF16)
        up_ref[...] = jnp.where(upper, dot(b, c, NT), 0.0).astype(BF16)
        high, low = split(jnp.where(lower, acc_ref[...], 0.0), 2)
        gc_ref[...] = dot(high, b) + dot(low, b)
        gb_ref[...] = dot(high, c, ((0,), (0,))) + dot(low, c, ((0,), (0,)))


def scores_part(first, segs, width, place, scaled, writer, reader, after):
    length, lanes = scaled[0].shape
    count = lanes // width
    _, turn, whole, proj = part_specs(length, width, segs, first)
    shape = jax.ShapeDtypeStruct
    return pl.pallas_call(
        functools.partial(scores_kernel, count, len(scaled) // 2),
        grid_spec=pltpu.PrefetchScalarGridSpec(
            num_scalar_prefetch=1,
            grid=(count,),
            in_specs=[pl.BlockSpec(memory_space=pl.ANY)]
            + [turn(length)] * len(scaled)
            + [proj, proj],
            out_specs=[whole(length, length)] * 2 + [whole(length, N)] * 2,
            scratch_shapes=[pltpu.VMEM((length, length), F32)],
        ),
        out_shape=[shape((length, length), BF16)] * 2 + [shape((length, N), F32)] * 2,
        cost_estimate=pl.CostEstimate(
            flops=4 * length * lanes * length, transcendentals=0, bytes_accessed=8 * length * lanes
        ),
    )(place, after, *scaled, writer, reader)


def tree_kernel(segs, place, parents, *refs):
    got, tails = refs[:segs], refs[segs : 2 * segs]
    sent = refs[2 * segs : 3 * segs]
    all_ref, end_ref, decay_ref, tail_ref = refs[3 * segs :]
    block = pl.program_id(0)
    for k in range(segs):
        seg = chunk_of(place, k)
        all_ref[seg] = got[k][...]
        decay_ref[seg] = tail_row(tails[k][...], block)
    end_ref[...] = jnp.zeros_like(end_ref)

    for seg in range(segs):
        parent = parents[seg]
        near = jnp.maximum(parent, 0)
        above = jnp.where(parent >= 0, parents[near], -1)

        @pl.when(parent >= 0)
        def _():
            end_ref[near] += all_ref[seg, N:, :].astype(F32)

        @pl.when(above >= 0)
        def _():
            end_ref[jnp.maximum(above, 0)] += decay_ref[near] * all_ref[seg, N:, :].astype(F32)

    rows = iota((EXTRA, LANES), 0)
    for k in range(segs):
        seg = chunk_of(place, k)
        parent = parents[seg]
        near = jnp.maximum(parent, 0)
        above = jnp.where(parent >= 0, parents[near], -1)
        state = all_ref[near, :N, :].astype(F32)
        lifted = decay_ref[near] * all_ref[jnp.maximum(above, 0), :N, :].astype(F32)
        start = jnp.where(parent >= 0, state, 0.0) + jnp.where(above >= 0, lifted, 0.0)
        start = start.astype(BF16)
        own = decay_ref[seg]
        end = (own * end_ref[seg]).astype(BF16)
        held = start.astype(F32) + all_ref[seg, :N, :].astype(F32) / own
        last = jnp.sum(end.astype(F32) * held, axis=0, keepdims=True)
        at = pl.multiple_of(block * 2 * N, 2 * N)
        sent[k][pl.ds(at, N), :] = start
        sent[k][pl.ds(pl.multiple_of(at + N, N), N), :] = end
        tail = tail_rows([(block, last)])
        tail_ref[k] = jnp.where(block == 0, tail, tail_ref[k] + tail)

    @pl.when(block == pl.num_programs(0) - 1)
    def _():
        for k in range(segs):
            sent[k][sent[k].shape[0] - EXTRA :, :] = tail_ref[k].astype(BF16)


def tree_chunk(segs, place, parents, messages):
    rows, _ = messages[0].shape
    blocks = (rows - EXTRA) // (2 * N)
    state = pl.BlockSpec((2 * N, LANES), lambda i, f, p: (i, 0))
    tail = pl.BlockSpec((EXTRA, LANES), lambda i, f, p: (2 * N * blocks // EXTRA, 0))
    return pl.pallas_call(
        functools.partial(tree_kernel, segs),
        grid_spec=pltpu.PrefetchScalarGridSpec(
            num_scalar_prefetch=2,
            grid=(blocks,),
            in_specs=[state] * segs + [tail] * segs,
            out_specs=[pl.BlockSpec((rows, LANES), lambda i, f, p: (0, 0))] * segs,
            scratch_shapes=[
                pltpu.VMEM((segs, 2 * N, LANES), BF16),
                pltpu.VMEM((segs, N, LANES), F32),
                pltpu.VMEM((segs, 1, LANES), F32),
                pltpu.VMEM((segs, EXTRA, LANES), F32),
            ],
        ),
        out_shape=[jax.ShapeDtypeStruct((rows, LANES), BF16)] * segs,
        cost_estimate=pl.CostEstimate(flops=10**7, transcendentals=0, bytes_accessed=10**7),
        name="tree",
    )(place, parents, *messages, *messages)


def unpack(messages, state_ref, last_ref):
    blocks = state_ref.shape[1] // LANES // len(messages)
    for at, message in enumerate(messages):
        tail = message[2 * N * blocks :, :]
        for block in range(blocks):
            lane = (at * blocks + block) * LANES
            cols = slice(lane, lane + LANES)
            state_ref[:, cols] = message[2 * N * block : 2 * N * (block + 1), :]
            if last_ref is not None:
                last_ref[:, cols] = tail_row(tail, block)


def grads_shapes(length, heads):
    if heads:
        return [jax.ShapeDtypeStruct((2, length // heads, N), BF16)] * heads
    return [jax.ShapeDtypeStruct((length, N), F32)] * 2


def give(place, outs, accb_ref, accc_ref):
    if outs[0].dtype == F32:
        outs[0][...] = accb_ref[...]
        outs[1][...] = accc_ref[...]
        return
    block = accb_ref.shape[0] // len(outs)
    for k, out in enumerate(outs):
        row = jnp.bitwise_xor(place[0], k) * block
        rows = pl.ds(pl.multiple_of(row, block), block)
        out[0] = accb_ref[rows, :].astype(BF16)
        out[1] = accc_ref[rows, :].astype(BF16)


def grads_kernel(count, place, *refs):
    messages, refs = refs[:count], refs[count:]
    xs_ref, ys_ref, gb_in, gc_in, *outs, accb_ref, accc_ref, state_ref = refs
    step = pl.program_id(0)

    @pl.when(step == 0)
    def _():
        accb_ref[...] = gb_in[...]
        accc_ref[...] = gc_in[...]

    for at in range(count):

        @pl.when(step == at)
        def _(message=messages[at]):
            unpack([message], state_ref, None)

    accc_ref[...] += dot(ys_ref[...], state_ref[:N, :], NT)
    accb_ref[...] += dot(xs_ref[...], state_ref[N:, :], NT)

    @pl.when(step == count - 1)
    def _():
        give(place, outs, accb_ref, accc_ref)


def grads_part(first, piece, segs, width, heads, place, messages, xs, ys, gb, gc):
    length, lanes = xs.shape
    count = lanes // width
    _, turn, whole, _ = part_specs(length, width, segs, first, PIECES, piece)
    outs = grads_shapes(length, heads)
    return pl.pallas_call(
        functools.partial(grads_kernel, count),
        grid_spec=pltpu.PrefetchScalarGridSpec(
            num_scalar_prefetch=1,
            grid=(count,),
            in_specs=[whole(*messages[0].shape)] * len(messages)
            + [turn(length)] * 2
            + [whole(length, N)] * 2,
            out_specs=[whole(*out.shape) for out in outs],
            scratch_shapes=[pltpu.VMEM((length, N), F32)] * 2 + [pltpu.VMEM((2 * N, width // PIECES), BF16)],
        ),
        out_shape=outs,
        cost_estimate=pl.CostEstimate(
            flops=4 * length * count * width * N,
            transcendentals=0,
            bytes_accessed=8 * length * count * width,
        ),
    )(place, *messages, xs, ys, gb, gc)


def outputs_kernel(first, piece, per, count, earlier, final, grads, place, *refs):
    messages, refs = refs[: count * per], refs[count * per :]
    x_ref, dy_ref, xs_ref, ys_ref, table_ref, low_ref, up_ref, b_ref, c_ref, skip_ref = refs[:10]
    refs = refs[10:]
    if earlier:
        sums_in, _, _, *refs = refs
    if final:
        delta_ref, rate_ref, *refs = refs
    if grads:
        gb_in, gc_in, *refs = refs
    out_ref, dx_ref, end_ref, *refs = refs
    *refs, state_ref, last_ref = refs
    sums_ref = refs.pop() if final else end_ref
    if grads:
        *outs, accb_ref, accc_ref = refs
    step = pl.program_id(0)
    length, width = x_ref.shape
    for at in range(count):

        @pl.when(step == at)
        def _(parts=messages[at * per : (at + 1) * per]):
            unpack(parts, state_ref, last_ref)

    @pl.when(step == 0)
    def _():
        if grads:
            accb_ref[...] = gb_in[...]
            accc_ref[...] = gc_in[...]
        sums_ref[...] = sums_in[...] if earlier else jnp.zeros_like(sums_ref)

    chunk = chunk_of(place, step + first)
    for at in range(0, width, TILE):
        cols = slice(at, at + TILE)
        lane = (chunk * (PIECES // per) + piece) * width + at
        lanes = spread_at(lane)
        fall = dot(table_ref[0], lanes)
        grow = dot(table_ref[1], lanes)
        xs, ys = xs_ref[:, cols], ys_ref[:, cols]
        start, end = state_ref[:N, cols], state_ref[N:, cols]
        core = dot(low_ref[...], xs) + dot(c_ref[...], start)
        grad = dot(up_ref[...], ys) + dot(b_ref[...], end)
        skip = skip_ref[:, cols]
        out_ref[:, cols] = (fall * core + skip * x_ref[:, cols].astype(F32)).astype(BF16)
        dx_ref[:, cols] = (grow * grad + skip * dy_ref[:, cols].astype(F32)).astype(BF16)
        if grads:
            accc_ref[...] += dot(ys, start, NT)
            accb_ref[...] += dot(xs, end, NT)
        direct = xs.astype(F32) * grad
        through = ys.astype(F32) * core - direct
        shape = (TILE, 2 * SLOTS)
        column = iota(shape, 1)
        head = (lane + iota(shape, 0)) // P_SIZE
        pick_through = onehot(column == head)
        pick_direct = onehot(column == head + SLOTS)
        high, low = split(through, 2)
        dhigh, dlow = split(direct, 2)
        rows = dot(high, pick_through) + dot(low, pick_through)
        sums_ref[...] += rows + dot(dhigh, pick_direct) + dot(dlow, pick_direct)
        at_last = jnp.where(iota((8, TILE), 0) == 7, last_ref[:, cols], 0.0)
        high, low = split(at_last, 2)
        sums_ref[length - 8 :, :] += dot(high, pick_through) + dot(low, pick_through)

    if grads:

        @pl.when(step == count - 1)
        def _():
            give(place, outs, accb_ref, accc_ref)

    if final:

        @pl.when(step == count - 1)
        def _():
            rate = jnp.concatenate([rate_ref[...], jnp.ones_like(rate_ref)], axis=1)
            both = (sums_ref[...] * rate).T
            square = (length, length)
            later = onehot(iota(square, 0) >= iota(square, 1))
            back = sum(dot(piece, later) for piece in split(both[:SLOTS], 3))
            end_ref[...] = both[SLOTS:] / delta_ref[...] - back


def outputs_part(first, piece, per, segs, place, messages, x, dy, xs, ys, table, low, up, skip, writer, reader, earlier=(), final=(), grads=(), heads=0):
    length, lanes = x.shape
    width = lanes // segs
    count = len(messages) // per
    tile, turn, whole, proj = part_specs(
        length, width, segs, first, PIECES // per, piece
    )
    shape = jax.ShapeDtypeStruct
    sums = shape((length, 2 * SLOTS), F32)
    full = shape((length, lanes), BF16)
    any_ = pl.BlockSpec(memory_space=pl.ANY)
    in_specs = (
        [whole(*messages[0].shape)] * len(messages)
        + [tile(length), tile(length), turn(length), turn(length)]
        + [whole(*table.shape), whole(length, length), whole(length, length), proj, proj]
        + [tile(1)]
    )
    args = [*messages, x, dy, xs, ys, table, low, up, writer, reader, skip]
    aliases = {}
    if earlier:
        in_specs += [whole(*sums.shape), any_, any_]
        args += list(earlier)
        aliases = {len(args) - 1: 0, len(args): 1}
    in_specs += [whole(*value.shape) for value in (*final, *grads)]
    args += [*final, *grads]
    part = width * per // PIECES
    scratch = [pltpu.VMEM((2 * N, part), BF16), pltpu.VMEM((1, part), F32)]
    out_specs, out_shape = [tile(length), tile(length)], [full, full]
    end = shape(final[0].shape, F32) if final else sums
    out_specs.append(whole(*end.shape))
    out_shape.append(end)
    if final:
        scratch = [pltpu.VMEM(sums.shape, F32)] + scratch
    if grads:
        scratch = [pltpu.VMEM((length, N), F32)] * 2 + scratch
        given = grads_shapes(length, heads)
        out_specs += [whole(*value.shape) for value in given]
        out_shape += given
    return pl.pallas_call(
        functools.partial(
            outputs_kernel, first, piece, per, count, bool(earlier), bool(final), bool(grads)
        ),
        grid_spec=pltpu.PrefetchScalarGridSpec(
            num_scalar_prefetch=1,
            grid=(count,),
            in_specs=in_specs,
            out_specs=out_specs,
            scratch_shapes=scratch,
        ),
        out_shape=out_shape,
        input_output_aliases=aliases,
        cost_estimate=pl.CostEstimate(
            flops=12 * length * count * width * length,
            transcendentals=0,
            bytes_accessed=16 * length * count * width,
        ),
    )(place, *args)


def place_kernel(heads, segs, place, *refs):
    near, far, (gb_ref, gc_ref) = refs[:heads], refs[heads : 2 * heads], refs[2 * heads :]
    for k in range(heads):
        owner = jnp.bitwise_xor(place[0], k)
        for half, parts in enumerate((near, far)):
            group = 2 * owner + group_of(chunk_of(place, half * segs // 2), segs)
            cols = pl.ds(pl.multiple_of(group * N, N), N)
            gb_ref[:, cols] = parts[k][0]
            gc_ref[:, cols] = parts[k][1]


def place_grads(segs, place, near, far):
    heads = len(near)
    rows = near[0].shape[1]
    shape = jax.ShapeDtypeStruct((rows, 2 * heads * N), BF16)
    return pl.pallas_call(
        functools.partial(place_kernel, heads, segs),
        grid_spec=pltpu.PrefetchScalarGridSpec(
            num_scalar_prefetch=1,
            grid=(1,),
            in_specs=[pl.BlockSpec(near[0].shape, lambda i, f: (0, 0, 0))] * (2 * heads),
            out_specs=[pl.BlockSpec(shape.shape, lambda i, f: (0, 0))] * 2,
        ),
        out_shape=[shape] * 2,
        name="place_grads",
    )(place, *near, *far)


def swap(value, axis, k):
    size = lax.axis_size(axis)
    return lax.ppermute(value, axis, [(i, i ^ k) for i in range(size)])


def paired(inputs, deltas, rates, skips, writer, reader, grad_out, parents):
    segs = lax.axis_size("seg")
    heads = lax.axis_size("head")
    mid, late = segs // 2, 3 * segs // 4
    near_ks, mid_ks, late_ks = range(mid), range(mid, late), range(late, segs)
    place = jnp.stack([lax.axis_index("head"), lax.axis_index("seg")]).astype(jnp.int32)
    x, dy, b, c = inputs[0], grad_out[0], writer[0], reader[0]
    width = x.shape[1] // segs
    delta = deltas[0]
    own, got, back = {}, {}, {}

    def keep(ks, messages):
        for at, message in enumerate(messages):
            own[ks[at // PIECES], at % PIECES] = message

    def move(out, values, ks, piece):
        for k in ks:
            out[k, piece] = swap(values[k, piece], "seg", k) if k else values[k, piece]

    def arrived(ks, pieces):
        return [back[k, piece] for k in ks for piece in pieces]

    *parts, xs1, ys1, table = states_part(
        mid, late - mid, segs, place, x, dy, (delta, rates[None, :]), b, c
    )
    keep(mid_ks, parts)
    move(got, own, mid_ks, 0)
    *parts, xs2, ys2 = states_part(late, segs - late, segs, place, x, dy, (table,), b, c)
    keep(late_ks, parts)
    move(got, own, late_ks, 0)
    *parts, xs0, ys0 = states_part(0, mid, segs, place, x, dy, (table,), b, c)
    keep(near_ks, parts)
    move(got, own, near_ks, 0)
    for piece in range(1, PIECES):
        move(got, own, mid_ks, piece)
        move(got, own, late_ks, piece)
        move(got, own, near_ks, piece)
    skip = jnp.repeat(skips, P_SIZE)[None, :]
    scaled = (xs1, ys1, xs2, ys2)
    low1, up1, gb1, gc1 = scores_part(mid, segs, width, place, scaled, b, c, skip)
    low0, up0, gb0, gc0 = scores_part(0, segs, width, place, (xs0, ys0), b, c, skip)
    for piece in range(PIECES):
        sent = tree_chunk(segs, place, parents, [got[k, piece] for k in range(segs)])
        sent = {(k, piece): value for k, value in enumerate(sent)}
        move(back, sent, near_ks, piece)
        move(back, sent, mid_ks, piece)
        move(back, sent, late_ks, piece)
    near = (0, near_ks, xs0, ys0, low0, up0)
    middle = (mid, mid_ks, xs1, ys1, low1, up1)
    last = (late, late_ks, xs2, ys2, low1, up1)
    so_far = ()

    def outputs(chunks, pieces, **more):
        nonlocal so_far
        first, ks, xs, ys, low, up = chunks
        out, dx, sums, *grads = outputs_part(
            first,
            pieces[0],
            len(pieces),
            segs,
            place,
            arrived(ks, pieces),
            x,
            dy,
            xs,
            ys,
            table,
            low,
            up,
            skip,
            b,
            c,
            earlier=so_far,
            **more,
        )
        so_far = (sums, out, dx)
        return grads

    both = range(PIECES)
    grads0 = outputs(near, both, grads=(gb0, gc0), heads=heads)
    moved0 = [grads0[0]] + [swap(grads0[k], "head", k) for k in range(1, heads)]
    gb1, gc1 = outputs(last, (0,), grads=(gb1, gc1))
    gb1, gc1 = outputs(middle, both, grads=(gb1, gc1))
    grads1 = grads_part(
        late, 1, segs, width, heads, place, arrived(late_ks, (1,)), xs2, ys2, gb1, gc1
    )
    moved1 = [grads1[0]] + [swap(grads1[k], "head", k) for k in range(1, heads)]
    outputs(last, (1,), final=(delta, rates[None, :]))
    dd, out, dx = so_far
    gb, gc = place_grads(segs, place, moved0, moved1)
    return out[None], dx[None], dd[None], gb[None], gc[None]


def power_of_two(size):
    return size & (size - 1) == 0


def shards(inputs, deltas, rates, skips, writer, reader, grad_out, parents, levels):
    heads = deltas.shape[1]
    per_group_all = H // G
    local_groups = max(1, heads // per_group_all)
    members = max(1, per_group_all // heads)
    segs = lax.axis_size("seg")
    lanes = inputs.shape[2]
    even = power_of_two(segs) and power_of_two(lax.axis_size("head")) and segs >= 4
    if even and local_groups == 2 and heads == SLOTS and lanes // segs % TILE == 0:
        return paired(inputs, deltas, rates, skips, writer, reader, grad_out, parents)
    first_group = (lax.axis_index("head") * heads // per_group_all).astype(jnp.int32)[None]
    x, dy = inputs[0], grad_out[0]
    pad = SLOTS - heads
    delta = jnp.pad(deltas[0], ((0, pad), (0, 0)))
    rate = jnp.pad(rates, (0, pad))
    u, v, xs, ys, table, low, up, gb, gc = local_part(
        x, dy, delta, rate[None, :], writer[0], reader[0], first_group, local_groups
    )
    decay = jnp.repeat(jnp.exp(-rates * jnp.sum(deltas[0], axis=1)), P_SIZE)
    start, end = tree_states(u, v, decay, parents, levels)
    out, dx, gb, gc, dd = final_part(
        x,
        dy,
        xs,
        ys,
        start,
        end,
        u,
        table,
        low,
        up,
        gb,
        gc,
        jnp.repeat(skips, P_SIZE)[None, :],
        delta,
        rate[:, None],
        writer[0],
        reader[0],
        first_group,
        BF16 if members == 1 else F32,
    )
    grads = group_grads(gb, gc, members)
    return (out[None], dx[None], dd[None, :heads], grads[0][None], grads[1][None])


def solution(mesh):
    placed = (
        P("seg", None, "head"),
        P("seg", "head", None),
        P("head"),
        P("head"),
        P("seg", None, None),
        P("seg", None, None),
        P("seg", None, "head"),
        P(),
        P(),
    )
    return jax.shard_map(
        shards,
        mesh=mesh,
        in_specs=placed,
        out_specs=(
            P("seg", None, "head"),
            P("seg", None, "head"),
            P("seg", "head", None),
            P("seg", "head", None),
            P("seg", "head", None),
        ),
        check_vma=False,
    )
```
